128 devices in a mesh: pts: 32 (over x, y, core), head: 4 (over z).
Axes of the slice: x: 4, y: 4, z: 4, core: 2. Of those that a mesh axis runs over, the one named last changes fastest.
Arguments:
- tokens: bfloat16 [65536, 1024], P(('pts', 'head')), may hold values from -6 to 6
- w_query: bfloat16 [1024, 1024], replicated, may hold values from -0.1875 to 0.1875
- w_key: bfloat16 [1024, 256], replicated, may hold values from -0.1875 to 0.1875
- w_value: bfloat16 [1024, 256], replicated, may hold values from -0.1875 to 0.1875
- w_out: bfloat16 [1024, 1024], replicated, may hold values from -0.1875 to 0.1875
- logit_scale: float32 [16], replicated, may hold values from 1 to 64
- w_gate: bfloat16 [1024, 2048], replicated, may hold values from -0.1875 to 0.1875
- w_up: bfloat16 [1024, 2048], replicated, may hold values from -0.1875 to 0.1875
- w_down: bfloat16 [2048, 1024], replicated, may hold values from -0.125 to 0.125
- picks: int32 [512, 4], P('pts'), may hold values from 0 to 511, as said below
Outputs:
- mixed: bfloat16 [65536, 1024], P(('pts', 'head'))
The draws below stay inside these ranges and needn't reach their ends.
Inputs may be any that keep to these rules, and one draw needn't show every extreme that they name: `picks`: each row names 4 different blocks, none of them held by the row's own index of pts (block id // 16). Among the rows of one index of pts, at most 2 different blocks of any other index are named, and exactly 2 for some index.
All inputs are finite; a program needn't handle non-finite values.
Results may differ from the reference program's by a relative error of at most 0.0095.
The reference program's roundings to bfloat16 on the way count: a program that leaves them out, or rounds other values in their place, can miss the bound.
Values may be sent and summed in bfloat16 or wider, within the bound.
No kernel may reach another device: no remote copies, remote signals or barrier semaphores. Data moves between devices by JAX's collectives and lax.ppermute only.
A program may use at most 128 MiB of HBM per device.

```python
import math
import jax
import jax.numpy as jnp
from jax import lax

D = 1024
HEADS = 16
KV_HEADS = 4
HEAD_DIM = 64
FFN_UNITS = 2048
BALL = 256
BLOCK = 128
CMP = 64
PICKS = 4
CAP = 2
BLK_DEV = 16
NBLK = 512
TOKENS = 65536
NCMP = 1024


def draw_logit_scale(key, part):
    first = jax.random.fold_in(key, 0)
    levels = jnp.exp(jax.random.uniform(first, (HEADS,), jnp.float32, 0.0, math.log(8.0)))
    return levels.astype(jnp.float32)


def draw_picks(key, part):
    owners = NBLK // BLK_DEV
    pieces = jax.random.split(key, 4)
    popular = jax.random.randint(pieces[0], (owners,), 0, 4)
    noise = jax.random.randint(pieces[1], (NBLK, owners), 0, 64)
    columns = jnp.arange(owners)
    device_of = jnp.arange(NBLK) // BLK_DEV
    ranking = (noise + 48 * popular[None, :]) * owners + columns[None, :]
    ranking = jnp.where(columns[None, :] == device_of[:, None], -1, ranking)
    ranked = lax.top_k(ranking, PICKS)[1].astype(jnp.int32)
    base = jax.random.randint(pieces[2], (owners, owners), 0, BLK_DEV)
    advance = jax.random.randint(pieces[3], (NBLK, PICKS), 0, CAP)
    leading = (jnp.arange(NBLK) % BLK_DEV == 0)[:, None]
    position = jnp.arange(PICKS)[None, :] * jnp.ones((NBLK, 1), jnp.int32)
    lead_owner = jnp.take_along_axis(ranked, jnp.maximum(position - (CAP - 1), 0), axis=1)
    owner_ids = jnp.where(leading, lead_owner, ranked)
    lead_step = jnp.where(position < CAP, position, advance)
    step_ids = jnp.where(leading, lead_step, advance)
    offsets = (base[device_of[:, None] * jnp.ones((1, PICKS), jnp.int32), owner_ids] + step_ids) % BLK_DEV
    return (owner_ids * BLK_DEV + offsets).astype(jnp.int32)


def block_scale(key, shape, shards, smallest, top_value):
    def one(dim, blocks):
        heights = jax.random.uniform(jax.random.fold_in(jax.random.fold_in(key, 6), dim), (blocks,), jnp.float32, smallest / len(shards), top_value / len(shards))
        return jnp.repeat(jnp.exp(heights), shape[dim] // blocks).reshape((-1,) + (1,) * (len(shape) - dim - 1))

    gain = one(*shards[0])
    for cut in shards[1:]:
        gain = gain * one(*cut)
    return gain


def bell_draw(own_key, extent, spread, most, cuts=(), kind=jnp.bfloat16):
    values = spread * jax.random.normal(own_key, extent, jnp.float32)
    if cuts:
        values = values * block_scale(own_key, extent, cuts, -0.22, 0.18)
    return jnp.clip(values, -most, most).astype(kind)


def setup_inputs(seed: int = 0) -> dict:
    splits = jax.random.split(jax.random.key(seed), 11)
    tokens = bell_draw(splits[0], (TOKENS, D), 1.0, 6.0, ((0, 128),))
    w_query = bell_draw(splits[1], (D, HEADS * HEAD_DIM), D ** -0.5, 0.1875)
    w_key = bell_draw(splits[2], (D, KV_HEADS * HEAD_DIM), D ** -0.5, 0.1875)
    w_value = bell_draw(splits[3], (D, KV_HEADS * HEAD_DIM), D ** -0.5, 0.1875)
    w_out = bell_draw(splits[4], (HEADS * HEAD_DIM, D), (HEADS * HEAD_DIM) ** -0.5, 0.1875)
    logit_scale = draw_logit_scale(jax.random.fold_in(splits[10], 71), 0)
    w_gate = bell_draw(splits[6], (D, FFN_UNITS), D ** -0.5, 0.1875)
    w_up = bell_draw(splits[7], (D, FFN_UNITS), D ** -0.5, 0.1875)
    w_down = bell_draw(splits[8], (FFN_UNITS, D), FFN_UNITS ** -0.5, 0.125)
    picks = draw_picks(jax.random.fold_in(splits[10], 71), 0)
    return {"tokens": tokens, "w_query": w_query, "w_key": w_key, "w_value": w_value, "w_out": w_out, "logit_scale": logit_scale, "w_gate": w_gate, "w_up": w_up, "w_down": w_down, "picks": picks}


EPS = 1e-06

def rms_rows(values_in):
    return values_in * lax.rsqrt(lax.optimization_barrier(jnp.mean(values_in * values_in, axis=-1, keepdims=True)) + EPS)

def widened(values_in):
    return lax.optimization_barrier(values_in).astype(jnp.float32)

def reference(tokens, w_query, w_key, w_value, w_out, logit_scale, w_gate, w_up, w_down, picks):
    rows_all = tokens.shape[0]
    ratio = HEADS // KV_HEADS
    per_ball = BALL // BLOCK
    normed = rms_rows(tokens.astype(jnp.float32)).astype(jnp.bfloat16)
    queries = jnp.dot(normed, w_query, preferred_element_type=jnp.float32).reshape(rows_all, HEADS, HEAD_DIM)
    query_hat = rms_rows(queries).astype(jnp.bfloat16)
    keys_raw = jnp.dot(normed, w_key, preferred_element_type=jnp.float32).reshape(rows_all, KV_HEADS, HEAD_DIM)
    key_hat = rms_rows(keys_raw).astype(jnp.bfloat16)
    value = jnp.dot(normed, w_value, preferred_element_type=jnp.float32).astype(jnp.bfloat16).reshape(rows_all, KV_HEADS, HEAD_DIM)
    key_wide = widened(key_hat)
    value_wide = widened(value)
    summary_key = rms_rows(lax.optimization_barrier(jnp.mean(key_wide.reshape(NCMP, CMP, KV_HEADS, HEAD_DIM), axis=1))).astype(jnp.bfloat16)
    summary_value = lax.optimization_barrier(jnp.mean(value_wide.reshape(NCMP, CMP, KV_HEADS, HEAD_DIM), axis=1)).astype(jnp.bfloat16)
    summary_key = widened(summary_key)
    summary_value = widened(summary_value)
    key_blocks = key_wide.reshape(NBLK, BLOCK, KV_HEADS, HEAD_DIM)
    value_blocks = value_wide.reshape(NBLK, BLOCK, KV_HEADS, HEAD_DIM)
    query_wide = widened(query_hat)
    factor = (logit_scale.astype(jnp.float32) / math.sqrt(HEAD_DIM)).reshape(KV_HEADS, ratio, 1, 1)

    def one_ball(index):
        start = index * BALL
        here = lax.dynamic_slice_in_dim(query_wide, start, BALL, 0).reshape(BALL, KV_HEADS, ratio, HEAD_DIM)
        near_keys = lax.dynamic_slice_in_dim(key_wide, start, BALL, 0)
        near_values = lax.dynamic_slice_in_dim(value_wide, start, BALL, 0)
        chosen = lax.dynamic_slice_in_dim(picks, index * per_ball, per_ball, 0)
        far_keys = key_blocks[chosen].reshape(per_ball, PICKS * BLOCK, KV_HEADS, HEAD_DIM)
        far_values = value_blocks[chosen].reshape(per_ball, PICKS * BLOCK, KV_HEADS, HEAD_DIM)
        score_ball = jnp.einsum('tgrd,kgd->grtk', here, near_keys) * factor
        score_cmp = jnp.einsum('tgrd,kgd->grtk', here, summary_key) * factor
        grouped = here.reshape(per_ball, BLOCK, KV_HEADS, ratio, HEAD_DIM)
        score_far = jnp.einsum('cqgrd,ckgd->grcqk', grouped, far_keys).reshape(KV_HEADS, ratio, BALL, PICKS * BLOCK) * factor
        peak = jnp.maximum(jnp.maximum(lax.optimization_barrier(jnp.max(score_ball, axis=-1)), lax.optimization_barrier(jnp.max(score_cmp, axis=-1))), lax.optimization_barrier(jnp.max(score_far, axis=-1)))[..., None]
        expo_ball = jnp.exp(score_ball - peak)
        expo_cmp = jnp.exp(score_cmp - peak)
        expo_far = jnp.exp(score_far - peak)
        totals = lax.optimization_barrier(jnp.sum(expo_ball, axis=-1)) + lax.optimization_barrier(jnp.sum(expo_cmp, axis=-1)) + lax.optimization_barrier(jnp.sum(expo_far, axis=-1))
        weight_ball = widened(expo_ball.astype(jnp.bfloat16))
        weight_cmp = widened(expo_cmp.astype(jnp.bfloat16))
        weight_far = widened(expo_far.astype(jnp.bfloat16)).reshape(KV_HEADS, ratio, per_ball, BLOCK, PICKS * BLOCK)
        summed = jnp.einsum('grtk,kgd->tgrd', weight_ball, near_values)
        summed = summed + jnp.einsum('grtk,kgd->tgrd', weight_cmp, summary_value)
        summed = summed + jnp.einsum('grcqk,ckgd->cqgrd', weight_far, far_values).reshape(BALL, KV_HEADS, ratio, HEAD_DIM)
        result = summed / jnp.transpose(totals, (2, 0, 1))[..., None]
        return result.reshape(BALL, HEADS * HEAD_DIM).astype(jnp.bfloat16)
    attended = lax.map(one_ball, jnp.arange(rows_all // BALL, dtype=jnp.int32)).reshape(rows_all, HEADS * HEAD_DIM)
    mid = tokens.astype(jnp.float32) + jnp.dot(attended, w_out, preferred_element_type=jnp.float32)
    normed_mid = rms_rows(mid).astype(jnp.bfloat16)
    gate = jnp.dot(normed_mid, w_gate, preferred_element_type=jnp.float32)
    upward = jnp.dot(normed_mid, w_up, preferred_element_type=jnp.float32)
    hidden = (jax.nn.silu(gate) * upward).astype(jnp.bfloat16)
    return (mid + jnp.dot(hidden, w_down, preferred_element_type=jnp.float32)).astype(jnp.bfloat16)
```

```python
import math

import jax
import jax.numpy as jnp
from jax import lax
from jax.experimental import pallas as pl
from jax.experimental.pallas import tpu as pltpu
from jax.sharding import PartitionSpec as P

HEADS = 16
KV_HEADS = 4
HEAD_DIM = 64
BALL = 256
BLOCK = 128
CMP = 64
PICKS = 4
CAP = 2
EPS = 1e-06
LOG2E = math.log2(math.e)

ROWS = 512
PTS = 32
ZS = 4
BLK_DEV = 16
GROUP_W = 256
PAIR_W = 128
SUM_LOCAL = ROWS // CMP
PAY_ROWS = KV_HEADS * SUM_LOCAL + 16
STATE = 80


bf16 = jnp.bfloat16
f32 = jnp.float32


def params(**kw):
    return pltpu.CompilerParams(vmem_limit_bytes=56 * 1024 * 1024, **kw)


def head_means(raw):
    width = raw.shape[1]
    r = lax.broadcasted_iota(jnp.int32, (width, width), 0) // HEAD_DIM
    c = lax.broadcasted_iota(jnp.int32, (width, width), 1) // HEAD_DIM
    ones = jnp.where(r == c, 1.0, 0.0).astype(bf16)
    squares = raw * raw
    high = squares.astype(bf16)
    low = (squares - high.astype(f32)).astype(bf16)
    sums = jnp.dot(high, ones, preferred_element_type=f32) + jnp.dot(
        low, ones, preferred_element_type=f32
    )
    return sums * (1.0 / HEAD_DIM)


def head_norm(raw):
    return raw * lax.rsqrt(head_means(raw) + EPS)


def row_norm(x):
    return x * lax.rsqrt(jnp.mean(x * x, axis=-1, keepdims=True) + EPS)


def kv_body(picks, tokens, w_key, w_value, normed, pairs, payload, slots, table):
    def clear(i, _):
        table[i] = -1
        return 0

    lax.fori_loop(0, PTS * CAP, clear, 0)

    def assign(i, _):
        pick = picks[i // PICKS, i % PICKS]
        owner = pick // BLK_DEV
        offset = pick % BLK_DEV
        first = table[owner * CAP]
        slot = jnp.where((first == offset) | (first == -1), 0, 1)
        table[owner * CAP + slot] = offset
        slots[i // PICKS, i % PICKS] = owner * CAP + slot
        return 0

    lax.fori_loop(0, BLK_DEV * PICKS, assign, 0)

    here = row_norm(tokens[...].astype(f32)).astype(bf16)
    normed[...] = here
    keys = head_norm(jnp.dot(here, w_key[...], preferred_element_type=f32)).astype(bf16)
    values = jnp.dot(here, w_value[...], preferred_element_type=f32).astype(bf16)
    key_mean = jnp.mean(keys.astype(f32).reshape(SUM_LOCAL, CMP, GROUP_W), axis=1)
    summary_key = head_norm(key_mean)
    summary_value = jnp.mean(values.astype(f32).reshape(SUM_LOCAL, CMP, GROUP_W), axis=1)
    pieces = []
    for g in range(KV_HEADS):
        lanes = slice(g * HEAD_DIM, (g + 1) * HEAD_DIM)
        pairs[g] = jnp.concatenate([keys[:, lanes], values[:, lanes]], axis=1)
        pieces.append(jnp.concatenate([summary_key[:, lanes], summary_value[:, lanes]], axis=1))
    summary = jnp.concatenate(pieces, axis=0).astype(bf16)
    lane = lax.broadcasted_iota(jnp.int32, (16, PAIR_W), 1)
    for o in range(PTS):
        payload[o, : KV_HEADS * SUM_LOCAL, :] = summary
        first = jnp.maximum(table[o * CAP], 0)
        second = jnp.maximum(table[o * CAP + 1], 0)
        asked = jnp.where(lane == 0, first, second).astype(f32).astype(bf16)
        payload[o, KV_HEADS * SUM_LOCAL :, :] = asked


def kv_stage(picks, tokens, w_key, w_value):
    return pl.pallas_call(
        kv_body,
        name="kv_stage",
        in_specs=[
            pl.BlockSpec(memory_space=pltpu.SMEM),
            pl.BlockSpec(memory_space=pltpu.VMEM),
            pl.BlockSpec(memory_space=pltpu.VMEM),
            pl.BlockSpec(memory_space=pltpu.VMEM),
        ],
        out_specs=[
            pl.BlockSpec(memory_space=pltpu.VMEM),
            pl.BlockSpec(memory_space=pltpu.VMEM),
            pl.BlockSpec(memory_space=pltpu.VMEM),
            pl.BlockSpec(memory_space=pltpu.SMEM),
        ],
        out_shape=[
            jax.ShapeDtypeStruct((ROWS, 1024), bf16),
            jax.ShapeDtypeStruct((KV_HEADS, ROWS, PAIR_W), bf16),
            jax.ShapeDtypeStruct((PTS, PAY_ROWS, PAIR_W), bf16),
            jax.ShapeDtypeStruct((BLK_DEV, PICKS), jnp.int32),
        ],
        scratch_shapes=[pltpu.SMEM((PTS * CAP,), jnp.int32)],
        compiler_params=params(),
        cost_estimate=pl.CostEstimate(
            flops=2 * ROWS * 1024 * 512, bytes_accessed=4 << 20, transcendentals=0
        ),
    )(picks, tokens, w_key, w_value)


def q_body(normed, w_query, out):
    raw = jnp.dot(normed[...], w_query[...], preferred_element_type=f32)
    out[0] = head_norm(raw).astype(bf16)


def q_stage(normed, w_query):
    return pl.pallas_call(
        q_body,
        name="q_stage",
        grid=(KV_HEADS,),
        in_specs=[
            pl.BlockSpec((ROWS, 1024), lambda g: (0, 0)),
            pl.BlockSpec((1024, GROUP_W), lambda g: (0, g)),
        ],
        out_specs=pl.BlockSpec((1, ROWS, GROUP_W), lambda g: (g, 0, 0)),
        out_shape=jax.ShapeDtypeStruct((KV_HEADS, ROWS, GROUP_W), bf16),
        compiler_params=params(),
        cost_estimate=pl.CostEstimate(
            flops=2 * ROWS * 1024 * 1024, bytes_accessed=4 << 20, transcendentals=0
        ),
    )(normed, w_query)


def reply_body(asked, z, c0, c1, c2, c3, out, held):
    for k, c in enumerate((c0, c1, c2, c3)):
        for b in range(ROWS // BLOCK):
            held[k * (ROWS // BLOCK) + b] = c[b * BLOCK : (b + 1) * BLOCK, :]
    per = ROWS // BLOCK

    def one(i, _):
        b = asked[i]
        k = lax.rem(z[0] - b // per + ZS, ZS)
        out[i] = held[k * per + b % per]
        return 0

    lax.fori_loop(0, PTS * CAP, one, 0, unroll=4)


def reply_stage(asked, z, chunks):
    return pl.pallas_call(
        reply_body,
        name="reply_stage",
        in_specs=[pl.BlockSpec(memory_space=pltpu.SMEM)] * 2
        + [pl.BlockSpec(memory_space=pltpu.VMEM)] * 4,
        out_specs=pl.BlockSpec(memory_space=pltpu.VMEM),
        out_shape=jax.ShapeDtypeStruct((PTS * CAP, BLOCK, PAIR_W), bf16),
        scratch_shapes=[pltpu.VMEM((BLK_DEV, BLOCK, PAIR_W), bf16)],
        compiler_params=params(),
    )(asked, z, *chunks)


def with_ones(kv):
    turned = jnp.transpose(kv[:, HEAD_DIM:])
    return jnp.concatenate([turned, jnp.ones((16, kv.shape[0]), kv.dtype)], axis=0)


def near_body(scale, q, kv, s0, s1, s2, s3, state):
    keys = [kv[...], s0[...], s1[...], s2[...], s3[...]]
    kv_all = jnp.concatenate(keys, axis=0)
    key_all = kv_all[:, :HEAD_DIM]
    val_all = with_ones(kv_all)
    for r in range(HEADS // KV_HEADS):
        here = q[:, r * HEAD_DIM : (r + 1) * HEAD_DIM]
        s = lax.dot_general(key_all, here, (((1,), (1,)), ((), ())), preferred_element_type=f32)
        peak = jnp.max(s, axis=0, keepdims=True)
        w = jnp.exp2((s - peak) * scale[r]).astype(bf16)
        o = jnp.dot(val_all, w, preferred_element_type=f32)
        state[0, r, : STATE - 8, :] = o[: STATE - 8]
        state[0, r, STATE - 8 :, :] = jnp.broadcast_to(peak, (8, BALL))


def near_stage(scale, q, kv, sums):
    return pl.pallas_call(
        near_body,
        name="near_stage",
        grid=(ROWS // BALL,),
        in_specs=[
            pl.BlockSpec(memory_space=pltpu.SMEM),
            pl.BlockSpec((BALL, GROUP_W), lambda b: (b, 0)),
            pl.BlockSpec((BALL, PAIR_W), lambda b: (b, 0)),
        ]
        + [pl.BlockSpec((PTS * SUM_LOCAL, PAIR_W), lambda b: (0, 0))] * 4,
        out_specs=pl.BlockSpec((1, 4, STATE, BALL), lambda b: (b, 0, 0, 0)),
        out_shape=jax.ShapeDtypeStruct((ROWS // BALL, 4, STATE, BALL), f32),
        compiler_params=params(),
        cost_estimate=pl.CostEstimate(
            flops=8 * 4 * ROWS * 1280 * 64, bytes_accessed=2 << 20, transcendentals=0
        ),
    )(scale, q, kv, *sums)


def far_body(slots, scale, q, state, b0, b1, b2, b3, out):
    kv_all = jnp.concatenate([b0[0], b1[0], b2[0], b3[0]], axis=0)
    key_all = kv_all[:, :HEAD_DIM]
    val_all = with_ones(kv_all)
    lane = lax.broadcasted_iota(jnp.int32, (1, 2 * BLOCK), 1)
    turned = []
    for r in range(0, HEADS // KV_HEADS, 2):
        here = jnp.concatenate(
            [q[:, (r + i) * HEAD_DIM : (r + i + 1) * HEAD_DIM] for i in range(2)], axis=0
        )
        held = jnp.concatenate([state[0, r], state[0, r + 1]], axis=1)
        factor = jnp.where(lane < BLOCK, scale[r], scale[r + 1])
        s = lax.dot_general(key_all, here, (((1,), (1,)), ((), ())), preferred_element_type=f32)
        before = held[STATE - 8 : STATE - 7]
        peak = jnp.maximum(jnp.max(s, axis=0, keepdims=True), before)
        w = jnp.exp2((s - peak) * factor).astype(bf16)
        o = jnp.dot(val_all, w, preferred_element_type=f32)
        keep = jnp.exp2((before - peak) * factor)
        total = held[HEAD_DIM : HEAD_DIM + 1] * keep + o[HEAD_DIM : HEAD_DIM + 1]
        merged = (held[:HEAD_DIM] * keep + o[:HEAD_DIM]) * (1.0 / total)
        turned += [merged[:, :BLOCK], merged[:, BLOCK:]]
    out[...] = jnp.transpose(jnp.concatenate(turned, axis=0)).astype(bf16)


def far_stage(slots, scale, q, state, fetched):
    per = ROWS // BLOCK
    half = BALL // BLOCK

    def picked(j):
        return pl.BlockSpec((1, BLOCK, PAIR_W), lambda i, slots: (slots[i, j], 0, 0))

    return pl.pallas_call(
        far_body,
        name="far_stage",
        grid_spec=pltpu.PrefetchScalarGridSpec(
            num_scalar_prefetch=1,
            grid=(per,),
            in_specs=[
                pl.BlockSpec(memory_space=pltpu.SMEM),
                pl.BlockSpec((BLOCK, GROUP_W), lambda i, slots: (i, 0)),
                pl.BlockSpec(
                    (1, 4, STATE, BLOCK), lambda i, slots: (i // half, 0, 0, i % half)
                ),
            ]
            + [picked(j) for j in range(PICKS)],
            out_specs=pl.BlockSpec((BLOCK, GROUP_W), lambda i, slots: (i, 0)),
        ),
        out_shape=jax.ShapeDtypeStruct((ROWS, GROUP_W), bf16),
        compiler_params=params(),
        cost_estimate=pl.CostEstimate(
            flops=8 * 4 * ROWS * 512 * 64, bytes_accessed=4 << 20, transcendentals=0
        ),
    )(slots, scale, q, state, fetched, fetched, fetched, fetched)


FFN = 2048
UNIT = 256


def ffn_body(z, tokens, a0, a1, a2, a3, w_out, w_gate, w_up, w_down, out, acc, held):
    step = pl.program_id(0)

    @pl.when(step == 0)
    def _():
        mid = tokens[...].astype(f32)
        for k, a in enumerate((a0, a1, a2, a3)):
            start = lax.rem(z[0] + k, ZS) * GROUP_W
            mid = mid + jnp.dot(
                a[...], w_out[pl.ds(start, GROUP_W), :], preferred_element_type=f32
            )
        acc[...] = mid
        held[...] = row_norm(mid).astype(bf16)

    here = held[...]
    gate = jnp.dot(here, w_gate[...], preferred_element_type=f32)
    upward = jnp.dot(here, w_up[...], preferred_element_type=f32)
    hidden = (gate / (1.0 + jnp.exp(-gate)) * upward).astype(bf16)
    acc[...] += jnp.dot(hidden, w_down[...], preferred_element_type=f32)

    @pl.when(step == FFN // UNIT - 1)
    def _():
        out[...] = acc[...].astype(bf16)


def ffn_stage(z, tokens, parts, w_out, w_gate, w_up, w_down):
    whole = lambda j: (0, 0)
    return pl.pallas_call(
        ffn_body,
        name="ffn_stage",
        grid=(FFN // UNIT,),
        in_specs=[
            pl.BlockSpec(memory_space=pltpu.SMEM),
            pl.BlockSpec((ROWS, 1024), whole),
        ]
        + [pl.BlockSpec((ROWS, GROUP_W), whole)] * 4
        + [
            pl.BlockSpec((1024, 1024), whole),
            pl.BlockSpec((1024, UNIT), lambda j: (0, j)),
            pl.BlockSpec((1024, UNIT), lambda j: (0, j)),
            pl.BlockSpec((UNIT, 1024), lambda j: (j, 0)),
        ],
        out_specs=pl.BlockSpec((ROWS, 1024), whole),
        out_shape=jax.ShapeDtypeStruct((ROWS, 1024), bf16),
        scratch_shapes=[pltpu.VMEM((ROWS, 1024), f32), pltpu.VMEM((ROWS, 1024), bf16)],
        compiler_params=params(),
        cost_estimate=pl.CostEstimate(
            flops=2 * ROWS * 1024 * 7168, bytes_accessed=18 << 20, transcendentals=0
        ),
    )(z, tokens, *parts, w_out, w_gate, w_up, w_down)


def shift(array, k):
    return lax.ppermute(array, "head", [(i, (i + k) % ZS) for i in range(ZS)])


def on_device(tokens, w_query, w_key, w_value, w_out, logit_scale, w_gate, w_up, w_down, picks):
    z = lax.axis_index("head")
    zs = z.astype(jnp.int32).reshape(1)
    scale = lax.dynamic_slice_in_dim(logit_scale, z * 4, 4, 0) * (LOG2E / math.sqrt(HEAD_DIM))

    normed, pairs, payload, slots = kv_stage(picks, tokens, w_key, w_value)

    def to(array, k):
        return lax.dynamic_index_in_dim(array, (z + k) % ZS, 0, keepdims=False)

    kv = [to(pairs, 0)] + [shift(to(pairs, k), k) for k in range(1, ZS)]
    told = lax.all_to_all(payload, "pts", split_axis=0, concat_axis=0, tiled=True)
    query = q_stage(normed, w_query)
    asked = told[:, KV_HEADS * SUM_LOCAL, :CAP].astype(jnp.int32).reshape(-1)
    replies = reply_stage(asked, zs, kv)
    fetched = lax.all_to_all(
        replies.reshape(PTS, CAP * BLOCK, PAIR_W), "pts", split_axis=0, concat_axis=0, tiled=True
    ).reshape(PTS * CAP, BLOCK, PAIR_W)

    def summary_to(k):
        start = ((z + k) % ZS) * SUM_LOCAL
        return lax.dynamic_slice_in_dim(told, start, SUM_LOCAL, 1).reshape(-1, PAIR_W)

    sums = [summary_to(0)] + [shift(summary_to(k), k) for k in range(1, ZS)]
    q = [to(query, 0)] + [shift(to(query, k), k) for k in range(1, ZS)]

    per = ROWS // BLOCK
    parts = [None] * ZS
    states = [None] * ZS
    for k in (0, 1, 3, 2):
        states[k] = near_stage(scale, q[k], kv[k], sums)
    for k in (2, 1, 3, 0):
        own = lax.dynamic_slice_in_dim(slots, ((z - k) % ZS) * per, per, 0)
        attended = far_stage(own, scale, q[k], states[k], fetched)
        parts[k] = shift(attended, ZS - k) if k else attended
    return ffn_stage(zs, tokens, parts, w_out, w_gate, w_up, w_down)


def solution(mesh):
    placed = (P(("pts", "head"), None), P(), P(), P(), P(), P(), P(), P(), P(), P("pts", None))
    return jax.shard_map(
        on_device, mesh=mesh, in_specs=placed, out_specs=P(("pts", "head"), None), check_vma=False
    )
```

```python
import functools
import math

import jax
import jax.numpy as jnp
from jax import lax
from jax.experimental import pallas as pl
from jax.experimental.pallas import tpu as pltpu
from jax.sharding import PartitionSpec as P


HEADS = 16
KV_HEADS = 4
HEAD_DIM = 64
BALL = 256
BLOCK = 128
CMP = 64
PICKS = 4
CAP = 2
EPS = 1e-06
LOG2E = math.log2(math.e)

ROWS = 512
PTS = 32
ZS = 4
BLK_DEV = 16
GROUP_W = 256
PAIR_W = 128
RATIO = HEADS // KV_HEADS
SUM_LOCAL = ROWS // CMP
SUM_ROWS = KV_HEADS * SUM_LOCAL
PAY_ROWS = SUM_ROWS + 16
PER = ROWS // BLOCK
BALLS = ROWS // BALL
FFN = 2048
UNIT = 256
STEPS = 2


bf16 = jnp.bfloat16
f32 = jnp.float32
VMEM = pltpu.VMEM
SMEM = pltpu.SMEM
NT = (((1,), (1,)), ((), ()))


def whole(space):
    return pl.BlockSpec(memory_space=space)


def near_core(array):
    return pltpu.with_memory_space_constraint(array, VMEM)


def far_core(array):
    return pltpu.with_memory_space_constraint(array, pltpu.HBM)


def params(mib):
    return pltpu.CompilerParams(vmem_limit_bytes=mib * 1024 * 1024)


def cost(flops, moved):
    return pl.CostEstimate(flops=flops, bytes_accessed=moved, transcendentals=0)


def head_ones(width):
    r = lax.broadcasted_iota(jnp.int32, (width, width), 0) // HEAD_DIM
    c = lax.broadcasted_iota(jnp.int32, (width, width), 1) // HEAD_DIM
    return jnp.where(r == c, 1.0, 0.0).astype(bf16)


def head_norm(raw, ones):
    squares = raw * raw
    high = squares.astype(bf16)
    low = (squares - high.astype(f32)).astype(bf16)
    sums = jnp.dot(high, ones, preferred_element_type=f32) + jnp.dot(
        low, ones, preferred_element_type=f32
    )
    return raw * lax.rsqrt(sums * (1.0 / HEAD_DIM) + EPS)


def row_norm(x):
    return x * lax.rsqrt(jnp.mean(x * x, axis=-1, keepdims=True) + EPS)


def first_body(
    z, picks, tokens_in, key_in, value_in, query_in,
    c0, c1, c2, c3, q0, q1, q2, q3, payload_out, slots,
    table, tokens, w_key, w_value, w_query, normed, pairs, queries, payload, sems, out_sems,
):
    rows_n = ROWS // STEPS
    weight_copies = [
        pltpu.make_async_copy(key_in, w_key, sems.at[0]),
        pltpu.make_async_copy(value_in, w_value, sems.at[1]),
        pltpu.make_async_copy(query_in, w_query, sems.at[2]),
    ]
    token_copies = [
        pltpu.make_async_copy(
            tokens_in.at[pl.ds(i * rows_n, rows_n)],
            tokens.at[pl.ds(i * rows_n, rows_n)],
            sems.at[3 + i],
        )
        for i in range(STEPS)
    ]
    token_copies[0].start()
    weight_copies[0].start()
    weight_copies[1].start()
    for c in token_copies[1:]:
        c.start()
    weight_copies[2].start()

    def clear(i, _):
        table[i] = -1
        return 0

    lax.fori_loop(0, PTS * CAP, clear, 0, unroll=8)

    def assign(i, _):
        row = i // PICKS
        col = i % PICKS
        pick = picks[col, row]
        owner = pick // BLK_DEV
        offset = pick % BLK_DEV
        first = table[owner * CAP]
        slot = jnp.where((first == offset) | (first == -1), 0, 1)
        table[owner * CAP + slot] = offset
        slots[row, col] = owner * CAP + slot
        return 0

    lax.fori_loop(0, BLK_DEV * PICKS, assign, 0, unroll=4)

    ones = head_ones(GROUP_W)
    key_means, value_means = [], []
    for i in range(STEPS):
        rows = slice(i * rows_n, (i + 1) * rows_n)
        token_copies[i].wait()
        here = row_norm(tokens[rows].astype(f32)).astype(bf16)
        normed[rows] = here
        if i == 0:
            weight_copies[0].wait()
        keys = jnp.dot(here, w_key[...], preferred_element_type=f32)
        keys = head_norm(keys, ones).astype(bf16)
        if i == 0:
            weight_copies[1].wait()
        values = jnp.dot(here, w_value[...], preferred_element_type=f32).astype(bf16)
        runs = (rows_n // CMP, CMP, GROUP_W)
        key_means.append(jnp.mean(keys.astype(f32).reshape(runs), axis=1))
        value_means.append(jnp.mean(values.astype(f32).reshape(runs), axis=1))
        for g in range(KV_HEADS):
            lanes = slice(g * HEAD_DIM, (g + 1) * HEAD_DIM)
            pairs[g, rows] = jnp.concatenate([keys[:, lanes], values[:, lanes]], axis=1)
    for k, c in enumerate((c0, c1, c2, c3)):
        c[...] = pairs[(z[0] + k) % ZS]
    summary_key = head_norm(jnp.concatenate(key_means, axis=0), ones)
    summary_value = jnp.concatenate(value_means, axis=0)
    summary = jnp.concatenate(
        [
            jnp.concatenate(
                [
                    summary_key[:, g * HEAD_DIM : (g + 1) * HEAD_DIM],
                    summary_value[:, g * HEAD_DIM : (g + 1) * HEAD_DIM],
                ],
                axis=1,
            )
            for g in range(KV_HEADS)
        ],
        axis=0,
    ).astype(bf16)
    lane = lax.broadcasted_iota(jnp.int32, (16, PAIR_W), 1)
    for o in range(PTS):
        payload[o, :SUM_ROWS, :] = summary
        first = jnp.maximum(table[o * CAP], 0)
        second = jnp.maximum(table[o * CAP + 1], 0)
        payload[o, SUM_ROWS:, :] = jnp.where(lane == 0, first, second).astype(f32).astype(bf16)
    outs = [pltpu.make_async_copy(payload, payload_out, out_sems.at[ZS])]
    outs[0].start()
    weight_copies[2].wait()
    for k, out in enumerate((q0, q1, q2, q3)):
        start = pl.multiple_of(((z[0] + k) % ZS) * GROUP_W, GROUP_W)
        raw = jnp.dot(normed[...], w_query[:, pl.ds(start, GROUP_W)], preferred_element_type=f32)
        queries[k] = head_norm(raw, ones).astype(bf16)
        outs.append(pltpu.make_async_copy(queries.at[k], out, out_sems.at[k]))
        outs[-1].start()
    for c in outs:
        c.wait()


def first_stage(z, picks, tokens, w_key, w_value, w_query):
    hbm = whole(pltpu.HBM)
    return pl.pallas_call(
        first_body,
        name="first_stage",
        in_specs=[whole(SMEM), whole(SMEM), hbm, hbm, hbm, hbm],
        out_specs=[whole(VMEM)] * ZS + [hbm] * (ZS + 1) + [whole(SMEM)],
        out_shape=[VMEM((ROWS, PAIR_W), bf16)] * ZS
        + [pltpu.HBM((ROWS, GROUP_W), bf16)] * ZS
        + [
            pltpu.HBM((PTS, PAY_ROWS, PAIR_W), bf16),
            jax.ShapeDtypeStruct((BLK_DEV, PICKS), jnp.int32),
        ],
        scratch_shapes=[
            SMEM((PTS * CAP,), jnp.int32),
            VMEM((ROWS, 1024), bf16),
            VMEM((1024, GROUP_W), bf16),
            VMEM((1024, GROUP_W), bf16),
            VMEM((1024, 1024), bf16),
            VMEM((ROWS, 1024), bf16),
            VMEM((KV_HEADS, ROWS, PAIR_W), bf16),
            VMEM((ZS, ROWS, GROUP_W), bf16),
            VMEM((PTS, PAY_ROWS, PAIR_W), bf16),
            pltpu.SemaphoreType.DMA((3 + STEPS,)),
            pltpu.SemaphoreType.DMA((ZS + 1,)),
        ],
        compiler_params=params(24),
        cost_estimate=cost(2 * ROWS * 1024 * 1536, 8 << 20),
    )(z, picks, *[far_core(a) for a in (tokens, w_key, w_value, w_query)])


def reply_body(
    z, told, c0, c1, c2, c3, replies, s0, s1, s2, s3, kv_out, held, sums, asked_v, asked, sems, sum_sems
):
    asked_v[...] = told[:, SUM_ROWS, :].astype(f32).astype(jnp.int32)
    fetch = pltpu.make_async_copy(asked_v, asked, sum_sems.at[ZS])
    fetch.start()
    for k, c in enumerate((c0, c1, c2, c3)):
        held[k] = c[...].reshape(PER, BLOCK, PAIR_W)
    outs = [pltpu.make_async_copy(held, kv_out, sum_sems.at[ZS + 1])]
    fetch.wait()

    def copy(i):
        b = asked[i // CAP, i % CAP]
        k = (z[0] - b // PER + ZS) % ZS
        return pltpu.make_async_copy(held.at[k, b % PER], replies.at[i], sems.at[i])

    def start_one(i, _):
        copy(i).start()
        return 0

    def wait_one(i, _):
        copy(i).wait()
        return 0

    lax.fori_loop(0, PTS * CAP, start_one, 0, unroll=4)
    for k, s in enumerate((s0, s1, s2, s3)):
        start = pl.multiple_of(((z[0] + k) % ZS) * SUM_LOCAL, SUM_LOCAL)
        sums[k] = told[:, pl.ds(start, SUM_LOCAL), :].reshape(PTS * SUM_LOCAL, PAIR_W)
        outs.append(pltpu.make_async_copy(sums.at[k], s, sum_sems.at[k]))
    for c in outs:
        c.start()
    lax.fori_loop(0, PTS * CAP, wait_one, 0, unroll=4)
    for c in outs:
        c.wait()


def reply_stage(z, told, chunks):
    hbm = whole(pltpu.HBM)
    return pl.pallas_call(
        reply_body,
        name="reply_stage",
        in_specs=[whole(SMEM)] + [whole(VMEM)] * 5,
        out_specs=[hbm] * (ZS + 2),
        out_shape=[pltpu.HBM((PTS * CAP, BLOCK, PAIR_W), bf16)]
        + [pltpu.HBM((PTS * SUM_LOCAL, PAIR_W), bf16)] * ZS
        + [pltpu.HBM((ZS, PER, BLOCK, PAIR_W), bf16)],
        scratch_shapes=[
            VMEM((ZS, PER, BLOCK, PAIR_W), bf16),
            VMEM((ZS, PTS * SUM_LOCAL, PAIR_W), bf16),
            VMEM((PTS, PAIR_W), jnp.int32),
            SMEM((PTS, PAIR_W), jnp.int32),
            pltpu.SemaphoreType.DMA((PTS * CAP,)),
            pltpu.SemaphoreType.DMA((ZS + 2,)),
        ],
        compiler_params=params(8),
    )(z, near_core(told), *[near_core(c) for c in chunks])


def ones_beside(kv):
    return jnp.concatenate([jnp.ones((kv.shape[0], HEAD_DIM), kv.dtype), kv[:, HEAD_DIM:]], axis=1)


def near_body(chunk, z, scale, q, kv, s0, s1, s2, s3, *rest):
    state_out, held, state, sems = rest[-4:]
    lane = lax.broadcasted_iota(jnp.int32, (BALL, PAIR_W), 1)
    sums = jnp.concatenate([s0[...], s1[...], s2[...], s3[...]], axis=0)
    sum_keys = sums[:, :HEAD_DIM]
    sum_values = ones_beside(sums)
    half = BALL // BLOCK

    def ball_of(b):
        return kv[chunk, pl.ds(b * half, half)].reshape(BALL, PAIR_W)

    def scores(b, r, keys):
        here = q[pl.ds(b * BALL, BALL), r * HEAD_DIM : (r + 1) * HEAD_DIM]
        ball = lax.dot_general(here, keys, NT, preferred_element_type=f32)
        far = lax.dot_general(here, sum_keys, NT, preferred_element_type=f32)
        held[r % 2, :, :BALL] = ball
        held[r % 2, :, BALL:] = far
        return jnp.maximum(
            jnp.max(ball, axis=1, keepdims=True), jnp.max(far, axis=1, keepdims=True)
        )

    def copy(b, r):
        return pltpu.make_async_copy(state.at[b, r], state_out.at[b, r], sems.at[b, r])

    def one_ball(b, peak):
        ball = ball_of(b)
        values = ones_beside(ball)
        after = jnp.minimum(b + 1, BALLS - 1)
        for r in range(RATIO):
            if r + 1 < RATIO:
                coming = scores(b, r + 1, ball[:, :HEAD_DIM])
            else:
                coming = scores(after, 0, ball_of(after)[:, :HEAD_DIM])
            factor = scale[z[0] * RATIO + r] * (LOG2E / math.sqrt(HEAD_DIM))
            w = jnp.exp2((held[r % 2] - peak) * factor).astype(bf16)
            summed = jnp.dot(w[:, :BALL], values, preferred_element_type=f32) + jnp.dot(
                w[:, BALL:], sum_values, preferred_element_type=f32
            )
            state[b, r] = jnp.where(lane < HEAD_DIM // 2, peak, summed)
            copy(b, r).start()
            peak = coming
        return peak

    lax.fori_loop(0, BALLS, one_ball, scores(0, 0, ball_of(0)[:, :HEAD_DIM]))
    for b in range(BALLS):
        for r in range(RATIO):
            copy(b, r).wait()


def near_stage(chunk, z, scale, q, kv, sums, others):
    return pl.pallas_call(
        functools.partial(near_body, chunk),
        name="near_stage",
        in_specs=[whole(SMEM)] * 2 + [whole(VMEM)] * 6 + [whole(pl.ANY)] * len(others),
        out_specs=whole(pltpu.HBM),
        out_shape=pltpu.HBM((BALLS, RATIO, BALL, PAIR_W), f32),
        scratch_shapes=[
            VMEM((2, BALL, BALL + PTS * SUM_LOCAL * ZS), f32),
            VMEM((BALLS, RATIO, BALL, PAIR_W), f32),
            pltpu.SemaphoreType.DMA((BALLS, RATIO)),
        ],
        compiler_params=params(12),
        cost_estimate=cost(8 * 4 * ROWS * 1280 * 64, 2 << 20),
    )(z, scale, near_core(q), near_core(kv), *[near_core(s) for s in sums], *[far_core(a) for a in others])


def far_body(shift_by, z, slots, scale, q, state, fetched, *rest):
    out, held = rest[-2:]
    lane = lax.broadcasted_iota(jnp.int32, (BLOCK, PAIR_W), 1)
    first_row = ((z[0] - shift_by + ZS) % ZS) * PER

    def part(r):
        return slice(r * BLOCK, (r + 1) * BLOCK)

    def keys_of(i):
        return jnp.concatenate([fetched[slots[first_row + i, j]] for j in range(PICKS)], axis=0)

    def scores(i, slot):
        here = jnp.concatenate(
            [q[pl.ds(i * BLOCK, BLOCK), r * HEAD_DIM : (r + 1) * HEAD_DIM] for r in range(RATIO)],
            axis=0,
        )
        s = lax.dot_general(here, keys_of(i)[:, :HEAD_DIM], NT, preferred_element_type=f32)
        held[slot] = s
        return jnp.max(s, axis=1, keepdims=True)

    def finish(b, i, slot, peak):
        rows = slice(slot * BLOCK, (slot + 1) * BLOCK)
        weights, keeps = [], []
        for r in range(RATIO):
            factor = scale[z[0] * RATIO + r] * (LOG2E / math.sqrt(HEAD_DIM))
            before = jnp.broadcast_to(state[b, r, rows, :1], (BLOCK, PAIR_W))
            new = jnp.maximum(before, peak[part(r)])
            s = held[slot, part(r), :]
            weights.append(
                jnp.concatenate(
                    [
                        jnp.exp2((s[:, part(j)] - new) * factor).astype(bf16)
                        for j in range(PICKS)
                    ],
                    axis=1,
                )
            )
            keeps.append(jnp.exp2((before - new) * factor))
        o = jnp.dot(
            jnp.concatenate(weights, axis=0), ones_beside(keys_of(i)), preferred_element_type=f32
        )
        for r in range(0, RATIO, 2):
            even = state[b, r, rows, :] * keeps[r] + o[part(r)]
            odd = state[b, r + 1, rows, :] * keeps[r + 1] + o[part(r + 1)]
            at = HEAD_DIM // 2
            total = jnp.where(
                lane < HEAD_DIM,
                jnp.broadcast_to(even[:, at : at + 1], (BLOCK, PAIR_W)),
                jnp.broadcast_to(odd[:, at : at + 1], (BLOCK, PAIR_W)),
            )
            summed = jnp.where(lane < HEAD_DIM, pltpu.roll(even, HEAD_DIM, 1), odd)
            out[pl.ds(i * BLOCK, BLOCK), r * HEAD_DIM : (r + 2) * HEAD_DIM] = (
                summed / total
            ).astype(bf16)

    def one_ball(b, peak):
        coming = scores(2 * b + 1, 1)
        finish(b, 2 * b, 0, peak)
        after = scores(jnp.minimum(2 * b + 2, PER - 2), 0)
        finish(b, 2 * b + 1, 1, coming)
        return after

    lax.fori_loop(0, BALLS, one_ball, scores(0, 0))


def far_stage(shift_by, z, slots, scale, q, state, fetched, others):
    return pl.pallas_call(
        functools.partial(far_body, shift_by),
        name="far_stage",
        in_specs=[whole(SMEM)] * 3 + [whole(VMEM)] * 3 + [whole(pl.ANY)] * len(others),
        out_specs=whole(VMEM),
        out_shape=VMEM((ROWS, GROUP_W), bf16),
        scratch_shapes=[VMEM((2, RATIO * BLOCK, PICKS * BLOCK), f32)],
        compiler_params=params(12),
        cost_estimate=cost(8 * 4 * ROWS * 512 * 64, 4 << 20),
    )(z, slots, scale, near_core(q), near_core(state), near_core(fetched), *[far_core(a) for a in others])


def ffn_body(
    z, tokens, a0, a1, a2, a3, w_out, w_gate, w_up, down_in, out, mid_held, held, hidden, w_down, sem
):
    down = pltpu.make_async_copy(down_in, w_down, sem.at[0])
    down.start()
    mid = tokens[...].astype(f32)
    for k, a in enumerate((a0, a1, a2, a3)):
        start = pl.multiple_of(((z[0] + k) % ZS) * GROUP_W, GROUP_W)
        mid = mid + jnp.dot(a[...], w_out[pl.ds(start, GROUP_W), :], preferred_element_type=f32)
    mid_held[...] = mid
    held[...] = row_norm(mid).astype(bf16)
    for j in range(FFN // UNIT):
        cols = slice(j * UNIT, (j + 1) * UNIT)
        gate = jnp.dot(held[...], w_gate[:, cols], preferred_element_type=f32)
        upward = jnp.dot(held[...], w_up[:, cols], preferred_element_type=f32)
        hidden[:, cols] = (gate / (1.0 + jnp.exp(-gate)) * upward).astype(bf16)
    down.wait()
    out[...] = (
        mid_held[...] + jnp.dot(hidden[...], w_down[...], preferred_element_type=f32)
    ).astype(bf16)


def ffn_stage(z, tokens, parts, w_out, w_gate, w_up, w_down):
    return pl.pallas_call(
        ffn_body,
        name="ffn_stage",
        in_specs=[whole(SMEM)] + [whole(VMEM)] * 8 + [whole(pltpu.HBM)],
        out_specs=whole(VMEM),
        out_shape=jax.ShapeDtypeStruct((ROWS, 1024), bf16),
        scratch_shapes=[
            VMEM((ROWS, 1024), f32),
            VMEM((ROWS, 1024), bf16),
            VMEM((ROWS, FFN), bf16),
            VMEM((FFN, 1024), bf16),
            pltpu.SemaphoreType.DMA((1,)),
        ],
        compiler_params=params(24),
        cost_estimate=cost(2 * ROWS * 1024 * 7168, 18 << 20),
    )(z, *[near_core(a) for a in (tokens, *parts, w_out, w_gate, w_up)], far_core(w_down))


def shift(array, k):
    return lax.ppermute(array, "head", [(i, (i + k) % ZS) for i in range(ZS)])


def body(tokens, w_query, w_key, w_value, w_out, logit_scale, w_gate, w_up, w_down, picks):
    z = lax.axis_index("head").astype(jnp.int32).reshape(1)
    first = first_stage(z, picks.T, tokens, w_key, w_value, w_query)
    pairs, query, payload, slots = first[:ZS], first[ZS : 2 * ZS], first[2 * ZS], first[2 * ZS + 1]
    chunks = [pairs[0]] + [shift(pairs[k], k) for k in (1, 2, 3)]
    told = lax.all_to_all(payload, "pts", split_axis=0, concat_axis=0, tiled=True)
    replies, *sums, kv = reply_stage(z, told, chunks)
    replies = replies.reshape(PTS, CAP * BLOCK, PAIR_W)
    fetched = lax.all_to_all(replies, "pts", split_axis=0, concat_axis=0, tiled=True)
    fetched = fetched.reshape(PTS * CAP, BLOCK, PAIR_W)
    sums = [sums[0]] + [shift(sums[k], k) for k in (1, 2, 3)]
    q = [query[0], None, None, None]
    for k in (1, 3, 2):
        q[k] = shift(query[k], k)
    states = [None] * ZS
    done = []
    for k in (0, 1, 3, 2):
        states[k] = near_stage(k, z, logit_scale, q[k], kv, sums, done)
        done = [states[k]]
    parts = [None] * ZS
    for k in (2, 1, 3, 0):
        others = [states[2]] if k != 2 else []
        attended = far_stage(k, z, slots, logit_scale, q[k], states[k], fetched, others)
        parts[k] = shift(attended, ZS - k) if k else attended
    return ffn_stage(z, tokens, parts, w_out, w_gate, w_up, w_down)


def solution(mesh):
    placed = (P(("pts", "head"), None), P(), P(), P(), P(), P(), P(), P(), P(), P("pts", None))
    return jax.shard_map(
        body, mesh=mesh, in_specs=placed, out_specs=P(("pts", "head"), None), check_vma=False
    )
```

```python
import functools
import math

import jax
import jax.numpy as jnp
from jax import lax
from jax.experimental import pallas as pl
from jax.experimental.pallas import tpu as pltpu
from jax.sharding import PartitionSpec as P


HEADS = 16
KV_HEADS = 4
HEAD_DIM = 64
BALL = 256
BLOCK = 128
CMP = 64
PICKS = 4
CAP = 2
EPS = 1e-06
LOG2E = math.log2(math.e)

ROWS = 512
PTS = 32
ZS = 4
BLK_DEV = 16
GROUP_W = 256
PAIR_W = 128
RATIO = HEADS // KV_HEADS
SUM_LOCAL = ROWS // CMP
SUM_ROWS = KV_HEADS * SUM_LOCAL
PAY_ROWS = SUM_ROWS + 16
PER = ROWS // BLOCK
BALLS = ROWS // BALL
FFN = 2048
UNIT = 256
STEPS = 2


bf16 = jnp.bfloat16
f32 = jnp.float32
VMEM = pltpu.VMEM
SMEM = pltpu.SMEM
NT = (((1,), (1,)), ((), ()))


def whole(space):
    return pl.BlockSpec(memory_space=space)


def near_core(array):
    return pltpu.with_memory_space_constraint(array, VMEM)


def far_core(array):
    return pltpu.with_memory_space_constraint(array, pltpu.HBM)


def params(mib):
    return pltpu.CompilerParams(vmem_limit_bytes=mib * 1024 * 1024)


def cost(flops, moved):
    return pl.CostEstimate(flops=flops, bytes_accessed=moved, transcendentals=0)


def head_ones(width):
    r = lax.broadcasted_iota(jnp.int32, (width, width), 0) // HEAD_DIM
    c = lax.broadcasted_iota(jnp.int32, (width, width), 1) // HEAD_DIM
    return jnp.where(r == c, 1.0, 0.0).astype(bf16)


def head_norm(raw, ones):
    squares = raw * raw
    high = squares.astype(bf16)
    low = (squares - high.astype(f32)).astype(bf16)
    sums = jnp.dot(high, ones, preferred_element_type=f32) + jnp.dot(
        low, ones, preferred_element_type=f32
    )
    return raw * lax.rsqrt(sums * (1.0 / HEAD_DIM) + EPS)


def row_norm(x):
    return x * lax.rsqrt(jnp.mean(x * x, axis=-1, keepdims=True) + EPS)


def first_body(
    z, picks, tokens_in, key_in, value_in,
    c0, c1, c2, c3, payload_out, normed_out, slots,
    table, tokens, w_key, w_value, normed, pairs, payload, sems, out_sems,
):
    rows_n = ROWS // STEPS
    weight_copies = [
        pltpu.make_async_copy(key_in, w_key, sems.at[0]),
        pltpu.make_async_copy(value_in, w_value, sems.at[1]),
    ]
    token_copies = [
        pltpu.make_async_copy(
            tokens_in.at[pl.ds(i * rows_n, rows_n)],
            tokens.at[pl.ds(i * rows_n, rows_n)],
            sems.at[2 + i],
        )
        for i in range(STEPS)
    ]
    token_copies[0].start()
    weight_copies[0].start()
    weight_copies[1].start()
    for c in token_copies[1:]:
        c.start()

    def clear(i, _):
        table[i] = -1
        return 0

    lax.fori_loop(0, PTS * CAP, clear, 0, unroll=8)

    def assign(i, _):
        row = i // PICKS
        col = i % PICKS
        pick = picks[col, row]
        owner = pick // BLK_DEV
        offset = pick % BLK_DEV
        first = table[owner * CAP]
        slot = jnp.where((first == offset) | (first == -1), 0, 1)
        table[owner * CAP + slot] = offset
        slots[row, col] = owner * CAP + slot
        return 0

    lax.fori_loop(0, BLK_DEV * PICKS, assign, 0, unroll=4)

    ones = head_ones(GROUP_W)
    key_means, value_means, outs = [], [], []
    for i in range(STEPS):
        rows = pl.ds(i * rows_n, rows_n)
        token_copies[i].wait()
        here = row_norm(tokens[rows].astype(f32)).astype(bf16)
        normed[rows] = here
        outs.append(
            pltpu.make_async_copy(normed.at[rows], normed_out.at[rows], out_sems.at[i])
        )
        outs[-1].start()
        if i == 0:
            weight_copies[0].wait()
        keys = jnp.dot(here, w_key[...], preferred_element_type=f32)
        keys = head_norm(keys, ones).astype(bf16)
        if i == 0:
            weight_copies[1].wait()
        values = jnp.dot(here, w_value[...], preferred_element_type=f32).astype(bf16)
        runs = (rows_n // CMP, CMP, GROUP_W)
        key_means.append(jnp.mean(keys.astype(f32).reshape(runs), axis=1))
        value_means.append(jnp.mean(values.astype(f32).reshape(runs), axis=1))
        for g in range(KV_HEADS):
            lanes = slice(g * HEAD_DIM, (g + 1) * HEAD_DIM)
            pairs[g, rows] = jnp.concatenate([keys[:, lanes], values[:, lanes]], axis=1)
    for k, c in enumerate((c0, c1, c2, c3)):
        c[...] = pairs[(z[0] + k) % ZS]
    summary_key = head_norm(jnp.concatenate(key_means, axis=0), ones)
    summary_value = jnp.concatenate(value_means, axis=0)
    summary = jnp.concatenate(
        [
            jnp.concatenate(
                [
                    summary_key[:, g * HEAD_DIM : (g + 1) * HEAD_DIM],
                    summary_value[:, g * HEAD_DIM : (g + 1) * HEAD_DIM],
                ],
                axis=1,
            )
            for g in range(KV_HEADS)
        ],
        axis=0,
    ).astype(bf16)
    lane = lax.broadcasted_iota(jnp.int32, (16, PAIR_W), 1)
    for o in range(PTS):
        payload[o, :SUM_ROWS, :] = summary
        first = jnp.maximum(table[o * CAP], 0)
        second = jnp.maximum(table[o * CAP + 1], 0)
        payload[o, SUM_ROWS:, :] = jnp.where(lane == 0, first, second).astype(f32).astype(bf16)
    outs.append(pltpu.make_async_copy(payload, payload_out, out_sems.at[STEPS]))
    outs[-1].start()
    for c in outs:
        c.wait()


def first_stage(z, picks, tokens, w_key, w_value):
    hbm = whole(pltpu.HBM)
    return pl.pallas_call(
        first_body,
        name="first_stage",
        in_specs=[whole(SMEM), whole(SMEM), hbm, hbm, hbm],
        out_specs=[whole(VMEM)] * ZS + [hbm] * 2 + [whole(SMEM)],
        out_shape=[VMEM((ROWS, PAIR_W), bf16)] * ZS
        + [
            pltpu.HBM((PTS, PAY_ROWS, PAIR_W), bf16),
            pltpu.HBM((ROWS, 1024), bf16),
            jax.ShapeDtypeStruct((BLK_DEV, PICKS), jnp.int32),
        ],
        scratch_shapes=[
            SMEM((PTS * CAP,), jnp.int32),
            VMEM((ROWS, 1024), bf16),
            VMEM((1024, GROUP_W), bf16),
            VMEM((1024, GROUP_W), bf16),
            VMEM((ROWS, 1024), bf16),
            VMEM((KV_HEADS, ROWS, PAIR_W), bf16),
            VMEM((PTS, PAY_ROWS, PAIR_W), bf16),
            pltpu.SemaphoreType.DMA((2 + STEPS,)),
            pltpu.SemaphoreType.DMA((STEPS + 1,)),
        ],
        compiler_params=params(16),
        cost_estimate=cost(2 * ROWS * 1024 * 512, 4 << 20),
    )(z, picks, *[far_core(a) for a in (tokens, w_key, w_value)])


def q_body(z, normed_in, query_in, q0, q1, q2, q3, normed, w_query, queries, sems, out_sems):
    def columns(k):
        return pl.ds(pl.multiple_of(((z[0] + k) % ZS) * GROUP_W, GROUP_W), GROUP_W)

    ins = [pltpu.make_async_copy(normed_in, normed, sems.at[ZS])]
    for k in range(ZS):
        ins.append(pltpu.make_async_copy(query_in.at[:, columns(k)], w_query.at[k], sems.at[k]))
    for c in ins:
        c.start()
    ones = head_ones(GROUP_W)
    ins[0].wait()
    outs = []
    for k, out in enumerate((q0, q1, q2, q3)):
        ins[k + 1].wait()
        raw = jnp.dot(normed[...], w_query[k], preferred_element_type=f32)
        queries[k] = head_norm(raw, ones).astype(bf16)
        outs.append(pltpu.make_async_copy(queries.at[k], out, out_sems.at[k]))
        outs[-1].start()
    for c in outs:
        c.wait()


def q_stage(z, normed, w_query):
    hbm = whole(pltpu.HBM)
    return pl.pallas_call(
        q_body,
        name="q_stage",
        in_specs=[whole(SMEM), hbm, hbm],
        out_specs=[hbm] * ZS,
        out_shape=[pltpu.HBM((ROWS, GROUP_W), bf16)] * ZS,
        scratch_shapes=[
            VMEM((ROWS, 1024), bf16),
            VMEM((ZS, 1024, GROUP_W), bf16),
            VMEM((ZS, ROWS, GROUP_W), bf16),
            pltpu.SemaphoreType.DMA((ZS + 1,)),
            pltpu.SemaphoreType.DMA((ZS,)),
        ],
        compiler_params=params(16),
        cost_estimate=cost(2 * ROWS * 1024 * 1024, 4 << 20),
    )(z, far_core(normed), far_core(w_query))


def reply_body(
    z, told, c0, c1, c2, c3, replies, s0, s1, s2, s3, kv_out, held, sums, asked_v, asked, sems, sum_sems
):
    asked_v[...] = told[:, SUM_ROWS, :].astype(f32).astype(jnp.int32)
    fetch = pltpu.make_async_copy(asked_v, asked, sum_sems.at[ZS])
    fetch.start()
    for k, c in enumerate((c0, c1, c2, c3)):
        held[k] = c[...].reshape(PER, BLOCK, PAIR_W)
    outs = [pltpu.make_async_copy(held, kv_out, sum_sems.at[ZS + 1])]
    fetch.wait()

    def copy(i):
        b = asked[i // CAP, i % CAP]
        k = (z[0] - b // PER + ZS) % ZS
        return pltpu.make_async_copy(held.at[k, b % PER], replies.at[i], sems.at[i])

    def start_one(i, _):
        copy(i).start()
        return 0

    def wait_one(i, _):
        copy(i).wait()
        return 0

    lax.fori_loop(0, PTS * CAP, start_one, 0, unroll=4)
    for k, s in enumerate((s0, s1, s2, s3)):
        start = pl.multiple_of(((z[0] + k) % ZS) * SUM_LOCAL, SUM_LOCAL)
        sums[k] = told[:, pl.ds(start, SUM_LOCAL), :].reshape(PTS * SUM_LOCAL, PAIR_W)
        outs.append(pltpu.make_async_copy(sums.at[k], s, sum_sems.at[k]))
    for c in outs:
        c.start()
    lax.fori_loop(0, PTS * CAP, wait_one, 0, unroll=4)
    for c in outs:
        c.wait()


def reply_stage(z, told, chunks):
    hbm = whole(pltpu.HBM)
    return pl.pallas_call(
        reply_body,
        name="reply_stage",
        in_specs=[whole(SMEM)] + [whole(VMEM)] * 5,
        out_specs=[hbm] * (ZS + 2),
        out_shape=[pltpu.HBM((PTS * CAP, BLOCK, PAIR_W), bf16)]
        + [pltpu.HBM((PTS * SUM_LOCAL, PAIR_W), bf16)] * ZS
        + [pltpu.HBM((ZS, PER, BLOCK, PAIR_W), bf16)],
        scratch_shapes=[
            VMEM((ZS, PER, BLOCK, PAIR_W), bf16),
            VMEM((ZS, PTS * SUM_LOCAL, PAIR_W), bf16),
            VMEM((PTS, PAIR_W), jnp.int32),
            SMEM((PTS, PAIR_W), jnp.int32),
            pltpu.SemaphoreType.DMA((PTS * CAP,)),
            pltpu.SemaphoreType.DMA((ZS + 2,)),
        ],
        compiler_params=params(8),
    )(z, near_core(told), *[near_core(c) for c in chunks])


def ones_beside(kv):
    return jnp.concatenate([jnp.ones((kv.shape[0], HEAD_DIM), kv.dtype), kv[:, HEAD_DIM:]], axis=1)


def near_body(chunk, z, scale, q, kv, s0, s1, s2, s3, *rest):
    state_out, peak_out, held, state, peaks, sems, peak_sems = rest[-7:]
    sums = jnp.concatenate([s0[...], s1[...], s2[...], s3[...]], axis=0)
    sum_keys = sums[:, :HEAD_DIM]
    sum_values = ones_beside(sums)
    half = BALL // BLOCK

    def ball_of(b):
        return kv[chunk, pl.ds(b * half, half)].reshape(BALL, PAIR_W)

    def scores(b, r, keys):
        here = q[pl.ds(b * BALL, BALL), r * HEAD_DIM : (r + 1) * HEAD_DIM]
        ball = lax.dot_general(here, keys, NT, preferred_element_type=f32)
        far = lax.dot_general(here, sum_keys, NT, preferred_element_type=f32)
        held[r % 2, :, :BALL] = ball
        held[r % 2, :, BALL:] = far
        peak = jnp.maximum(
            jnp.max(ball, axis=1, keepdims=True), jnp.max(far, axis=1, keepdims=True)
        )
        return peak.astype(bf16).astype(f32)

    def copies(b, r):
        return (
            pltpu.make_async_copy(state.at[b, r], state_out.at[b, r], sems.at[b, r]),
            pltpu.make_async_copy(peaks.at[b, r], peak_out.at[b, r], peak_sems.at[b, r]),
        )

    def one_ball(b, peak):
        ball = ball_of(b)
        values = ones_beside(ball)
        after = jnp.minimum(b + 1, BALLS - 1)
        for r in range(RATIO):
            if r + 1 < RATIO:
                coming = scores(b, r + 1, ball[:, :HEAD_DIM])
            else:
                coming = scores(after, 0, ball_of(after)[:, :HEAD_DIM])
            factor = scale[z[0] * RATIO + r] * (LOG2E / math.sqrt(HEAD_DIM))
            w = jnp.exp2((held[r % 2] - peak) * factor).astype(bf16)
            peaks[b, r] = jnp.broadcast_to(peak, (BALL, PAIR_W)).astype(bf16)
            state[b, r] = jnp.dot(w[:, :BALL], values, preferred_element_type=f32) + jnp.dot(
                w[:, BALL:], sum_values, preferred_element_type=f32
            )
            for c in copies(b, r):
                c.start()
            peak = coming
        return peak

    lax.fori_loop(0, BALLS, one_ball, scores(0, 0, ball_of(0)[:, :HEAD_DIM]))
    for b in range(BALLS):
        for r in range(RATIO):
            for c in copies(b, r):
                c.wait()


def near_stage(chunk, z, scale, q, kv, sums, others):
    return pl.pallas_call(
        functools.partial(near_body, chunk),
        name="near_stage",
        in_specs=[whole(SMEM)] * 2 + [whole(VMEM)] * 6 + [whole(pl.ANY)] * len(others),
        out_specs=[whole(pltpu.HBM)] * 2,
        out_shape=[
            pltpu.HBM((BALLS, RATIO, BALL, PAIR_W), f32),
            pltpu.HBM((BALLS, RATIO, BALL, PAIR_W), bf16),
        ],
        scratch_shapes=[
            VMEM((2, BALL, BALL + PTS * SUM_LOCAL * ZS), f32),
            VMEM((BALLS, RATIO, BALL, PAIR_W), f32),
            VMEM((BALLS, RATIO, BALL, PAIR_W), bf16),
            pltpu.SemaphoreType.DMA((BALLS, RATIO)),
            pltpu.SemaphoreType.DMA((BALLS, RATIO)),
        ],
        compiler_params=params(12),
        cost_estimate=cost(8 * 4 * ROWS * 1280 * 64, 2 << 20),
    )(z, scale, near_core(q), near_core(kv), *[near_core(s) for s in sums], *[far_core(a) for a in others])


def far_body(shift_by, z, slots, scale, q, state, peaks, fetched, *rest):
    out, held = rest[-2:]
    lane = lax.broadcasted_iota(jnp.int32, (BLOCK, PAIR_W), 1)
    first_row = ((z[0] - shift_by + ZS) % ZS) * PER

    def part(r):
        return slice(r * BLOCK, (r + 1) * BLOCK)

    def keys_of(i):
        return jnp.concatenate([fetched[slots[first_row + i, j]] for j in range(PICKS)], axis=0)

    def scores(i, slot):
        here = jnp.concatenate(
            [q[pl.ds(i * BLOCK, BLOCK), r * HEAD_DIM : (r + 1) * HEAD_DIM] for r in range(RATIO)],
            axis=0,
        )
        s = lax.dot_general(here, keys_of(i)[:, :HEAD_DIM], NT, preferred_element_type=f32)
        held[slot] = s
        return jnp.max(s, axis=1, keepdims=True)

    def finish(b, i, slot, peak):
        rows = slice(slot * BLOCK, (slot + 1) * BLOCK)
        weights, keeps = [], []
        for r in range(RATIO):
            factor = scale[z[0] * RATIO + r] * (LOG2E / math.sqrt(HEAD_DIM))
            before = peaks[b, r, rows, :].astype(f32)
            new = jnp.maximum(before, peak[part(r)])
            s = held[slot, part(r), :]
            weights.append(
                jnp.concatenate(
                    [
                        jnp.exp2((s[:, part(j)] - new) * factor).astype(bf16)
                        for j in range(PICKS)
                    ],
                    axis=1,
                )
            )
            keeps.append(jnp.exp2((before - new) * factor))
        o = jnp.dot(
            jnp.concatenate(weights, axis=0), ones_beside(keys_of(i)), preferred_element_type=f32
        )
        for r in range(0, RATIO, 2):
            even = state[b, r, rows, :] * keeps[r] + o[part(r)]
            odd = state[b, r + 1, rows, :] * keeps[r + 1] + o[part(r + 1)]
            total = jnp.where(lane < HEAD_DIM, even, pltpu.roll(odd, HEAD_DIM, 1))
            summed = jnp.where(lane < HEAD_DIM, pltpu.roll(even, HEAD_DIM, 1), odd)
            out[pl.ds(i * BLOCK, BLOCK), r * HEAD_DIM : (r + 2) * HEAD_DIM] = (
                summed / total
            ).astype(bf16)

    def one_ball(b, peak):
        coming = scores(2 * b + 1, 1)
        finish(b, 2 * b, 0, peak)
        after = scores(2 * b + 2, 0) if b + 1 < BALLS else None
        finish(b, 2 * b + 1, 1, coming)
        return after

    peak = scores(0, 0)
    for b in range(BALLS):
        peak = one_ball(b, peak)


def far_stage(shift_by, z, slots, scale, q, state, fetched, others):
    return pl.pallas_call(
        functools.partial(far_body, shift_by),
        name="far_stage",
        in_specs=[whole(SMEM)] * 3 + [whole(VMEM)] * 4 + [whole(pl.ANY)] * len(others),
        out_specs=whole(VMEM),
        out_shape=VMEM((ROWS, GROUP_W), bf16),
        scratch_shapes=[VMEM((2, RATIO * BLOCK, PICKS * BLOCK), f32)],
        compiler_params=params(12),
        cost_estimate=cost(8 * 4 * ROWS * 512 * 64, 4 << 20),
    )(z, slots, scale, near_core(q), *[near_core(a) for a in state], near_core(fetched), *[far_core(a) for a in others])


def ffn_body(
    z, tokens, a0, a1, a2, a3, w_out, w_gate, w_up, down_in, out, mid_held, held, hidden, w_down, sem
):
    down = pltpu.make_async_copy(down_in, w_down, sem.at[0])
    down.start()
    mid = tokens[...].astype(f32)
    for k, a in enumerate((a0, a1, a2, a3)):
        start = pl.multiple_of(((z[0] + k) % ZS) * GROUP_W, GROUP_W)
        mid = mid + jnp.dot(a[...], w_out[pl.ds(start, GROUP_W), :], preferred_element_type=f32)
    mid_held[...] = mid
    held[...] = row_norm(mid).astype(bf16)
    for j in range(FFN // UNIT):
        cols = slice(j * UNIT, (j + 1) * UNIT)
        gate = jnp.dot(held[...], w_gate[:, cols], preferred_element_type=f32)
        upward = jnp.dot(held[...], w_up[:, cols], preferred_element_type=f32)
        hidden[:, cols] = (gate / (1.0 + jnp.exp(-gate)) * upward).astype(bf16)
    down.wait()
    out[...] = (
        mid_held[...] + jnp.dot(hidden[...], w_down[...], preferred_element_type=f32)
    ).astype(bf16)


def ffn_stage(z, tokens, parts, w_out, w_gate, w_up, w_down):
    return pl.pallas_call(
        ffn_body,
        name="ffn_stage",
        in_specs=[whole(SMEM)] + [whole(VMEM)] * 8 + [whole(pltpu.HBM)],
        out_specs=whole(VMEM),
        out_shape=jax.ShapeDtypeStruct((ROWS, 1024), bf16),
        scratch_shapes=[
            VMEM((ROWS, 1024), f32),
            VMEM((ROWS, 1024), bf16),
            VMEM((ROWS, FFN), bf16),
            VMEM((FFN, 1024), bf16),
            pltpu.SemaphoreType.DMA((1,)),
        ],
        compiler_params=params(24),
        cost_estimate=cost(2 * ROWS * 1024 * 7168, 18 << 20),
    )(z, *[near_core(a) for a in (tokens, *parts, w_out, w_gate, w_up)], far_core(w_down))


def shift(array, k):
    return lax.ppermute(array, "head", [(i, (i + k) % ZS) for i in range(ZS)])


def body(tokens, w_query, w_key, w_value, w_out, logit_scale, w_gate, w_up, w_down, picks):
    z = lax.axis_index("head").astype(jnp.int32).reshape(1)
    *pairs, payload, normed, slots = first_stage(z, picks.T, tokens, w_key, w_value)
    chunks = [pairs[0]] + [shift(pairs[k], k) for k in (1, 2, 3)]
    told = lax.all_to_all(payload, "pts", split_axis=0, concat_axis=0, tiled=True)
    query = q_stage(z, normed, w_query)
    replies, *sums, kv = reply_stage(z, told, chunks)
    replies = replies.reshape(PTS, CAP * BLOCK, PAIR_W)
    fetched = lax.all_to_all(replies, "pts", split_axis=0, concat_axis=0, tiled=True)
    fetched = fetched.reshape(PTS * CAP, BLOCK, PAIR_W)
    sums = [sums[0]] + [shift(sums[k], k) for k in (1, 2, 3)]
    q = [query[0], None, None, None]
    for k in (1, 3, 2):
        q[k] = shift(query[k], k)
    states = [None] * ZS
    done = []
    for k in (0, 1, 3, 2):
        states[k] = near_stage(k, z, logit_scale, q[k], kv, sums, done)
        done = states[k]
    parts = [None] * ZS
    for k in (2, 1, 3, 0):
        others = states[2] if k != 2 else []
        attended = far_stage(k, z, slots, logit_scale, q[k], states[k], fetched, others)
        parts[k] = shift(attended, ZS - k) if k else attended
    return ffn_stage(z, tokens, parts, w_out, w_gate, w_up, w_down)


def solution(mesh):
    placed = (P(("pts", "head"), None), P(), P(), P(), P(), P(), P(), P(), P(), P("pts", None))
    return jax.shard_map(
        body, mesh=mesh, in_specs=placed, out_specs=P(("pts", "head"), None), check_vma=False
    )
```

```python
import functools
import math

import jax
import jax.numpy as jnp
from jax import lax
from jax.experimental import pallas as pl
from jax.experimental.pallas import tpu as pltpu
from jax.sharding import PartitionSpec as P


HEADS = 16
KV_HEADS = 4
HEAD_DIM = 64
BALL = 256
BLOCK = 128
CMP = 64
PICKS = 4
CAP = 2
EPS = 1e-06
LOG2E = math.log2(math.e)

ROWS = 512
PTS = 32
ZS = 4
BLK_DEV = 16
GROUP_W = 256
PAIR_W = 128
RATIO = HEADS // KV_HEADS
SUM_LOCAL = ROWS // CMP
SUM_ROWS = KV_HEADS * SUM_LOCAL
PAY_ROWS = SUM_ROWS + 16
PER = ROWS // BLOCK
BALLS = ROWS // BALL
FFN = 2048
UNIT = 256
STEPS = 2
GROUPS = ((0,), (1,), (3, 2))


bf16 = jnp.bfloat16
f32 = jnp.float32
VMEM = pltpu.VMEM
SMEM = pltpu.SMEM
NT = (((1,), (1,)), ((), ()))


def whole(space):
    return pl.BlockSpec(memory_space=space)


def near_core(array):
    return pltpu.with_memory_space_constraint(array, VMEM)


def far_core(array):
    return pltpu.with_memory_space_constraint(array, pltpu.HBM)


def params(mib):
    return pltpu.CompilerParams(vmem_limit_bytes=mib * 1024 * 1024)


def cost(flops, moved):
    return pl.CostEstimate(flops=flops, bytes_accessed=moved, transcendentals=0)


def head_ones(width):
    r = lax.broadcasted_iota(jnp.int32, (width, width), 0) // HEAD_DIM
    c = lax.broadcasted_iota(jnp.int32, (width, width), 1) // HEAD_DIM
    return jnp.where(r == c, 1.0, 0.0).astype(bf16)


def head_norm(raw, ones):
    squares = raw * raw
    high = squares.astype(bf16)
    low = (squares - high.astype(f32)).astype(bf16)
    sums = jnp.dot(high, ones, preferred_element_type=f32) + jnp.dot(
        low, ones, preferred_element_type=f32
    )
    return raw * lax.rsqrt(sums * (1.0 / HEAD_DIM) + EPS)


def row_norm(x):
    return x * lax.rsqrt(jnp.mean(x * x, axis=-1, keepdims=True) + EPS)


def first_body(
    z, picks, tokens_in, key_in, value_in,
    c0, c1, c2, c3, payload_out, normed_out, slots,
    table, tokens, w_key, w_value, normed, pairs, payload, sems, out_sems,
):
    rows_n = ROWS // STEPS
    weight_copies = [
        pltpu.make_async_copy(key_in, w_key, sems.at[0]),
        pltpu.make_async_copy(value_in, w_value, sems.at[1]),
    ]
    token_copies = [
        pltpu.make_async_copy(
            tokens_in.at[pl.ds(i * rows_n, rows_n)],
            tokens.at[pl.ds(i * rows_n, rows_n)],
            sems.at[2 + i],
        )
        for i in range(STEPS)
    ]
    token_copies[0].start()
    weight_copies[0].start()
    weight_copies[1].start()
    for c in token_copies[1:]:
        c.start()

    def clear(i, _):
        table[i] = -1
        return 0

    lax.fori_loop(0, PTS * CAP, clear, 0, unroll=8)

    def assign(i, _):
        row = i // PICKS
        col = i % PICKS
        pick = picks[col, row]
        owner = pick // BLK_DEV
        offset = pick % BLK_DEV
        first = table[owner * CAP]
        slot = jnp.where((first == offset) | (first == -1), 0, 1)
        table[owner * CAP + slot] = offset
        slots[row, col] = owner * CAP + slot
        return 0

    lax.fori_loop(0, BLK_DEV * PICKS, assign, 0, unroll=4)

    ones = head_ones(GROUP_W)
    key_means, value_means, outs = [], [], []
    for i in range(STEPS):
        rows = pl.ds(i * rows_n, rows_n)
        token_copies[i].wait()
        here = row_norm(tokens[rows].astype(f32)).astype(bf16)
        normed[rows] = here
        outs.append(
            pltpu.make_async_copy(normed.at[rows], normed_out.at[rows], out_sems.at[i])
        )
        outs[-1].start()
        if i == 0:
            weight_copies[0].wait()
        keys = jnp.dot(here, w_key[...], preferred_element_type=f32)
        keys = head_norm(keys, ones).astype(bf16)
        if i == 0:
            weight_copies[1].wait()
        values = jnp.dot(here, w_value[...], preferred_element_type=f32).astype(bf16)
        runs = (rows_n // CMP, CMP, GROUP_W)
        key_means.append(jnp.mean(keys.astype(f32).reshape(runs), axis=1))
        value_means.append(jnp.mean(values.astype(f32).reshape(runs), axis=1))
        for g in range(KV_HEADS):
            lanes = slice(g * HEAD_DIM, (g + 1) * HEAD_DIM)
            pairs[g, rows] = jnp.concatenate([keys[:, lanes], values[:, lanes]], axis=1)
    for k, c in enumerate((c0, c1, c2, c3)):
        c[...] = pairs[(z[0] + k) % ZS]
    summary_key = head_norm(jnp.concatenate(key_means, axis=0), ones)
    summary_value = jnp.concatenate(value_means, axis=0)
    summary = jnp.concatenate(
        [
            jnp.concatenate(
                [
                    summary_key[:, g * HEAD_DIM : (g + 1) * HEAD_DIM],
                    summary_value[:, g * HEAD_DIM : (g + 1) * HEAD_DIM],
                ],
                axis=1,
            )
            for g in range(KV_HEADS)
        ],
        axis=0,
    ).astype(bf16)
    lane = lax.broadcasted_iota(jnp.int32, (16, PAIR_W), 1)
    for o in range(PTS):
        payload[o, :SUM_ROWS, :] = summary
        first = jnp.maximum(table[o * CAP], 0)
        second = jnp.maximum(table[o * CAP + 1], 0)
        payload[o, SUM_ROWS:, :] = jnp.where(lane == 0, first, second).astype(f32).astype(bf16)
    outs.append(pltpu.make_async_copy(payload, payload_out, out_sems.at[STEPS]))
    outs[-1].start()
    for c in outs:
        c.wait()


def first_stage(z, picks, tokens, w_key, w_value):
    hbm = whole(pltpu.HBM)
    return pl.pallas_call(
        first_body,
        name="first_stage",
        in_specs=[whole(SMEM), whole(SMEM), hbm, hbm, hbm],
        out_specs=[whole(VMEM)] * ZS + [hbm] * 2 + [whole(SMEM)],
        out_shape=[VMEM((ROWS, PAIR_W), bf16)] * ZS
        + [
            pltpu.HBM((PTS, PAY_ROWS, PAIR_W), bf16),
            pltpu.HBM((ROWS, 1024), bf16),
            jax.ShapeDtypeStruct((BLK_DEV, PICKS), jnp.int32),
        ],
        scratch_shapes=[
            SMEM((PTS * CAP,), jnp.int32),
            VMEM((ROWS, 1024), bf16),
            VMEM((1024, GROUP_W), bf16),
            VMEM((1024, GROUP_W), bf16),
            VMEM((ROWS, 1024), bf16),
            VMEM((KV_HEADS, ROWS, PAIR_W), bf16),
            VMEM((PTS, PAY_ROWS, PAIR_W), bf16),
            pltpu.SemaphoreType.DMA((2 + STEPS,)),
            pltpu.SemaphoreType.DMA((STEPS + 1,)),
        ],
        compiler_params=params(16),
        cost_estimate=cost(2 * ROWS * 1024 * 512, 4 << 20),
    )(z, picks, *[far_core(a) for a in (tokens, w_key, w_value)])


def q_body(z, normed_in, query_in, q0, q1, q2, q3, normed, w_query, queries, sems, out_sems):
    def columns(k):
        return pl.ds(pl.multiple_of(((z[0] + k) % ZS) * GROUP_W, GROUP_W), GROUP_W)

    ins = [pltpu.make_async_copy(normed_in, normed, sems.at[ZS])]
    for k in range(ZS):
        ins.append(pltpu.make_async_copy(query_in.at[:, columns(k)], w_query.at[k], sems.at[k]))
    for c in ins:
        c.start()
    ones = head_ones(GROUP_W)
    ins[0].wait()
    outs = []
    for k, out in enumerate((q0, q1, q2, q3)):
        ins[k + 1].wait()
        raw = jnp.dot(normed[...], w_query[k], preferred_element_type=f32)
        queries[k] = head_norm(raw, ones).astype(bf16)
        outs.append(pltpu.make_async_copy(queries.at[k], out, out_sems.at[k]))
        outs[-1].start()
    for c in outs:
        c.wait()


def q_stage(z, normed, w_query):
    hbm = whole(pltpu.HBM)
    return pl.pallas_call(
        q_body,
        name="q_stage",
        in_specs=[whole(SMEM), hbm, hbm],
        out_specs=[hbm] * ZS,
        out_shape=[pltpu.HBM((ROWS, GROUP_W), bf16)] * ZS,
        scratch_shapes=[
            VMEM((ROWS, 1024), bf16),
            VMEM((ZS, 1024, GROUP_W), bf16),
            VMEM((ZS, ROWS, GROUP_W), bf16),
            pltpu.SemaphoreType.DMA((ZS + 1,)),
            pltpu.SemaphoreType.DMA((ZS,)),
        ],
        compiler_params=params(16),
        cost_estimate=cost(2 * ROWS * 1024 * 1024, 4 << 20),
    )(z, far_core(normed), far_core(w_query))


def reply_body(
    z, told, c0, c1, c2, c3, replies, s0, s1, s2, s3, kv_out, held, sums, asked_v, asked, sems, sum_sems
):
    asked_v[...] = told[:, SUM_ROWS, :].astype(f32).astype(jnp.int32)
    fetch = pltpu.make_async_copy(asked_v, asked, sum_sems.at[ZS])
    fetch.start()
    for k, c in enumerate((c0, c1, c2, c3)):
        held[k] = c[...].reshape(PER, BLOCK, PAIR_W)
    outs = [pltpu.make_async_copy(held, kv_out, sum_sems.at[ZS + 1])]
    fetch.wait()

    def copy(i):
        b = asked[i // CAP, i % CAP]
        k = (z[0] - b // PER + ZS) % ZS
        return pltpu.make_async_copy(held.at[k, b % PER], replies.at[i], sems.at[i])

    def start_one(i, _):
        copy(i).start()
        return 0

    def wait_one(i, _):
        copy(i).wait()
        return 0

    lax.fori_loop(0, PTS * CAP, start_one, 0, unroll=4)
    for k, s in enumerate((s0, s1, s2, s3)):
        start = pl.multiple_of(((z[0] + k) % ZS) * SUM_LOCAL, SUM_LOCAL)
        sums[k] = told[:, pl.ds(start, SUM_LOCAL), :].reshape(PTS * SUM_LOCAL, PAIR_W)
        outs.append(pltpu.make_async_copy(sums.at[k], s, sum_sems.at[k]))
    for c in outs:
        c.start()
    lax.fori_loop(0, PTS * CAP, wait_one, 0, unroll=4)
    for c in outs:
        c.wait()


def reply_stage(z, told, chunks):
    hbm = whole(pltpu.HBM)
    return pl.pallas_call(
        reply_body,
        name="reply_stage",
        in_specs=[whole(SMEM)] + [whole(VMEM)] * 5,
        out_specs=[hbm] * (ZS + 2),
        out_shape=[pltpu.HBM((PTS * CAP, BLOCK, PAIR_W), bf16)]
        + [pltpu.HBM((PTS * SUM_LOCAL, PAIR_W), bf16)] * ZS
        + [pltpu.HBM((ZS, PER, BLOCK, PAIR_W), bf16)],
        scratch_shapes=[
            VMEM((ZS, PER, BLOCK, PAIR_W), bf16),
            VMEM((ZS, PTS * SUM_LOCAL, PAIR_W), bf16),
            VMEM((PTS, PAIR_W), jnp.int32),
            SMEM((PTS, PAIR_W), jnp.int32),
            pltpu.SemaphoreType.DMA((PTS * CAP,)),
            pltpu.SemaphoreType.DMA((ZS + 2,)),
        ],
        compiler_params=params(8),
    )(z, near_core(told), *[near_core(c) for c in chunks])


def ones_beside(kv):
    return jnp.concatenate([jnp.ones((kv.shape[0], HEAD_DIM), kv.dtype), kv[:, HEAD_DIM:]], axis=1)


def near_body(chunks, z, scale, kv, s0, s1, s2, s3, *rest):
    n = len(chunks)
    qs, outs = rest[:n], rest[-6 - 2 * n : -6]
    held, q, state, peaks, sems, peak_sems = rest[-6:]
    sums = jnp.concatenate([s0[...], s1[...], s2[...], s3[...]], axis=0)
    sum_keys = sums[:, :HEAD_DIM]
    sum_values = ones_beside(sums)
    half = BALL // BLOCK

    def copies(c, b, r):
        return (
            pltpu.make_async_copy(state.at[c, b, r], outs[2 * c].at[b, r], sems.at[c, b, r]),
            pltpu.make_async_copy(peaks.at[c, b, r], outs[2 * c + 1].at[b, r], peak_sems.at[c, b, r]),
        )

    def one_chunk(c, here_of, chunk, start_copies):
        balls = [kv[chunk, pl.ds(b * half, half)].reshape(BALL, PAIR_W) for b in range(BALLS)]
        values = [ones_beside(ball) for ball in balls]
        units = [(b, r) for b in range(BALLS) for r in range(RATIO)]

        def scores(u):
            b, r = units[u]
            here = here_of(b, r)
            ball = lax.dot_general(
                here, balls[b][:, :HEAD_DIM], NT, preferred_element_type=f32
            )
            far = lax.dot_general(here, sum_keys, NT, preferred_element_type=f32)
            held[u % 2, :, :BALL] = ball
            held[u % 2, :, BALL:] = far
            peak = jnp.maximum(
                jnp.max(ball, axis=1, keepdims=True), jnp.max(far, axis=1, keepdims=True)
            )
            return peak.astype(bf16).astype(f32)

        peak = scores(0)
        for u, (b, r) in enumerate(units):
            coming = scores(u + 1) if u + 1 < len(units) else None
            factor = scale[z[0] * RATIO + r] * (LOG2E / math.sqrt(HEAD_DIM))
            w = jnp.exp2((held[u % 2] - peak) * factor).astype(bf16)
            peaks[c, b, r] = jnp.broadcast_to(peak, (BALL, PAIR_W)).astype(bf16)
            state[c, b, r] = jnp.dot(w[:, :BALL], values[b], preferred_element_type=f32) + jnp.dot(
                w[:, BALL:], sum_values, preferred_element_type=f32
            )
            start_copies(b, r)
            peak = coming

    def part(ref):
        def take(b, r):
            return ref[b * BALL : (b + 1) * BALL, r * HEAD_DIM : (r + 1) * HEAD_DIM]

        return take

    if n == 1:

        def begin(b, r):
            for c in copies(0, b, r):
                c.start()

        one_chunk(0, part(qs[0]), chunks[0], begin)
    else:

        def loop(c, _):
            for i in range(n):

                @pl.when(c == i)
                def _():
                    q[...] = qs[i][...]

            chunk = jnp.where(c == 0, chunks[0], chunks[1])
            one_chunk(c, part(q), chunk, lambda b, r: None)
            for i in range(n):

                @pl.when(c == i)
                def _():
                    for b in range(BALLS):
                        for r in range(RATIO):
                            for m in copies(i, b, r):
                                m.start()

            return 0

        lax.fori_loop(0, n, loop, 0)
    for c in range(n):
        for b in range(BALLS):
            for r in range(RATIO):
                for m in copies(c, b, r):
                    m.wait()


def near_stage(chunks, z, scale, qs, kv, sums, others):
    n = len(chunks)
    shape = (BALLS, RATIO, BALL, PAIR_W)
    outs = pl.pallas_call(
        functools.partial(near_body, chunks),
        name="near_stage",
        in_specs=[whole(SMEM)] * 2 + [whole(VMEM)] * (5 + n) + [whole(pl.ANY)] * len(others),
        out_specs=[whole(pltpu.HBM)] * (2 * n),
        out_shape=[pltpu.HBM(shape, f32), pltpu.HBM(shape, bf16)] * n,
        scratch_shapes=[
            VMEM((2, BALL, BALL + PTS * SUM_LOCAL * ZS), f32),
            VMEM((ROWS if n > 1 else 16, GROUP_W), bf16),
            VMEM((n, *shape), f32),
            VMEM((n, *shape), bf16),
            pltpu.SemaphoreType.DMA((n, BALLS, RATIO)),
            pltpu.SemaphoreType.DMA((n, BALLS, RATIO)),
        ],
        compiler_params=params(14),
        cost_estimate=cost(8 * 4 * n * ROWS * 1280 * 64, 2 << 20),
    )(
        z,
        scale,
        near_core(kv),
        *[near_core(s) for s in sums],
        *[near_core(q) for q in qs],
        *[far_core(a) for a in others],
    )
    return [outs[2 * c : 2 * c + 2] for c in range(n)]


def far_body(shift_by, direct, z, slots, scale, q, state, peaks, fetched, *rest):
    if direct:
        out, held, state_held, peaks_held, sems = rest[-5:]
        brought = []
        for b in range(BALLS):
            brought.append(
                (
                    pltpu.make_async_copy(state.at[b], state_held.at[b], sems.at[b, 0]),
                    pltpu.make_async_copy(peaks.at[b], peaks_held.at[b], sems.at[b, 1]),
                )
            )
            for c in brought[-1]:
                c.start()
        state, peaks = state_held, peaks_held
    else:
        out, held = rest[-2:]
    lane = lax.broadcasted_iota(jnp.int32, (BLOCK, PAIR_W), 1)
    first_row = ((z[0] - shift_by + ZS) % ZS) * PER

    def part(r):
        return slice(r * BLOCK, (r + 1) * BLOCK)

    def keys_of(i):
        return jnp.concatenate([fetched[slots[first_row + i, j]] for j in range(PICKS)], axis=0)

    def scores(i, slot):
        here = jnp.concatenate(
            [q[pl.ds(i * BLOCK, BLOCK), r * HEAD_DIM : (r + 1) * HEAD_DIM] for r in range(RATIO)],
            axis=0,
        )
        s = lax.dot_general(here, keys_of(i)[:, :HEAD_DIM], NT, preferred_element_type=f32)
        held[slot] = s
        return jnp.max(s, axis=1, keepdims=True)

    def finish(b, i, slot, peak):
        rows = slice(slot * BLOCK, (slot + 1) * BLOCK)
        weights, keeps = [], []
        for r in range(RATIO):
            factor = scale[z[0] * RATIO + r] * (LOG2E / math.sqrt(HEAD_DIM))
            before = peaks[b, r, rows, :].astype(f32)
            new = jnp.maximum(before, peak[part(r)])
            s = held[slot, part(r), :]
            weights.append(
                jnp.concatenate(
                    [
                        jnp.exp2((s[:, part(j)] - new) * factor).astype(bf16)
                        for j in range(PICKS)
                    ],
                    axis=1,
                )
            )
            keeps.append(jnp.exp2((before - new) * factor))
        o = jnp.dot(
            jnp.concatenate(weights, axis=0), ones_beside(keys_of(i)), preferred_element_type=f32
        )
        for r in range(0, RATIO, 2):
            even = state[b, r, rows, :] * keeps[r] + o[part(r)]
            odd = state[b, r + 1, rows, :] * keeps[r + 1] + o[part(r + 1)]
            total = jnp.where(lane < HEAD_DIM, even, pltpu.roll(odd, HEAD_DIM, 1))
            summed = jnp.where(lane < HEAD_DIM, pltpu.roll(even, HEAD_DIM, 1), odd)
            out[pl.ds(i * BLOCK, BLOCK), r * HEAD_DIM : (r + 2) * HEAD_DIM] = (
                summed / total
            ).astype(bf16)

    def one_ball(b, peak):
        coming = scores(2 * b + 1, 1)
        finish(b, 2 * b, 0, peak)
        after = scores(2 * b + 2, 0) if b + 1 < BALLS else None
        if direct and b + 1 < BALLS:
            for c in brought[b + 1]:
                c.wait()
        finish(b, 2 * b + 1, 1, coming)
        return after

    peak = scores(0, 0)
    if direct:
        for c in brought[0]:
            c.wait()
    for b in range(BALLS):
        peak = one_ball(b, peak)


def far_stage(shift_by, z, slots, scale, q, state, fetched, others, direct=False):
    shape = (BALLS, RATIO, BALL, PAIR_W)
    place, keep = (pltpu.HBM, far_core) if direct else (VMEM, near_core)
    extra = [VMEM(shape, f32), VMEM(shape, bf16), pltpu.SemaphoreType.DMA((BALLS, 2))]
    return pl.pallas_call(
        functools.partial(far_body, shift_by, direct),
        name="far_stage",
        in_specs=[whole(SMEM)] * 3
        + [whole(VMEM)]
        + [whole(place)] * 2
        + [whole(VMEM)]
        + [whole(pl.ANY)] * len(others),
        out_specs=whole(VMEM),
        out_shape=VMEM((ROWS, GROUP_W), bf16),
        scratch_shapes=[VMEM((2, RATIO * BLOCK, PICKS * BLOCK), f32)] + (extra if direct else []),
        compiler_params=params(12),
        cost_estimate=cost(8 * 4 * ROWS * 512 * 64, 4 << 20),
    )(
        z,
        slots,
        scale,
        near_core(q),
        *[keep(a) for a in state],
        near_core(fetched),
        *[far_core(a) for a in others],
    )


def ffn_body(z, tokens, a0, a1, a2, a3, w_out, w_gate, w_up, w_down, out, mid_held, held, hidden):
    mid = tokens[...].astype(f32)
    for k, a in enumerate((a0, a1, a2, a3)):
        start = pl.multiple_of(((z[0] + k) % ZS) * GROUP_W, GROUP_W)
        mid = mid + jnp.dot(a[...], w_out[pl.ds(start, GROUP_W), :], preferred_element_type=f32)
    mid_held[...] = mid
    held[...] = row_norm(mid).astype(bf16)
    for j in range(FFN // UNIT):
        cols = slice(j * UNIT, (j + 1) * UNIT)
        gate = jnp.dot(held[...], w_gate[:, cols], preferred_element_type=f32)
        upward = jnp.dot(held[...], w_up[:, cols], preferred_element_type=f32)
        hidden[:, cols] = (gate / (1.0 + jnp.exp(-gate)) * upward).astype(bf16)
    out[...] = (
        mid_held[...] + jnp.dot(hidden[...], w_down[...], preferred_element_type=f32)
    ).astype(bf16)


def ffn_stage(z, tokens, parts, w_out, w_gate, w_up, w_down):
    return pl.pallas_call(
        ffn_body,
        name="ffn_stage",
        in_specs=[whole(SMEM)] + [whole(VMEM)] * 9,
        out_specs=whole(VMEM),
        out_shape=jax.ShapeDtypeStruct((ROWS, 1024), bf16),
        scratch_shapes=[VMEM((ROWS, 1024), f32), VMEM((ROWS, 1024), bf16), VMEM((ROWS, FFN), bf16)],
        compiler_params=params(14),
        cost_estimate=cost(2 * ROWS * 1024 * 7168, 18 << 20),
    )(z, *[near_core(a) for a in (tokens, *parts, w_out, w_gate, w_up, w_down)])


def shift(array, k):
    return lax.ppermute(array, "head", [(i, (i + k) % ZS) for i in range(ZS)])


def body(tokens, w_query, w_key, w_value, w_out, logit_scale, w_gate, w_up, w_down, picks):
    z = lax.axis_index("head").astype(jnp.int32).reshape(1)
    *pairs, payload, normed, slots = first_stage(z, picks.T, tokens, w_key, w_value)
    chunks = [pairs[0]] + [shift(pairs[k], k) for k in (1, 2, 3)]
    told = lax.all_to_all(payload, "pts", split_axis=0, concat_axis=0, tiled=True)
    query = q_stage(z, normed, w_query)
    replies, *sums, kv = reply_stage(z, told, chunks)
    replies = replies.reshape(PTS, CAP * BLOCK, PAIR_W)
    fetched = lax.all_to_all(replies, "pts", split_axis=0, concat_axis=0, tiled=True)
    fetched = fetched.reshape(PTS * CAP, BLOCK, PAIR_W)
    sums = [sums[0]] + [shift(sums[k], k) for k in (1, 2, 3)]
    q = [query[0], None, None, None]
    for k in (1, 3, 2):
        q[k] = shift(query[k], k)
    states = [None] * ZS
    done = []
    for group in GROUPS:
        made = near_stage(group, z, logit_scale, [q[k] for k in group], kv, sums, done)
        for k, one in zip(group, made):
            states[k] = one
        done = made[-1]
    parts = [None] * ZS
    for k in (2, 1, 3, 0):
        others = states[2] if k != 2 else []
        attended = far_stage(k, z, slots, logit_scale, q[k], states[k], fetched, others, k == 2)
        parts[k] = shift(attended, ZS - k) if k else attended
    return ffn_stage(z, tokens, parts, w_out, w_gate, w_up, w_down)


def solution(mesh):
    placed = (P(("pts", "head"), None), P(), P(), P(), P(), P(), P(), P(), P(), P("pts", None))
    return jax.shard_map(
        body, mesh=mesh, in_specs=placed, out_specs=P(("pts", "head"), None), check_vma=False
    )
```

```python
import functools
import math

import jax
import jax.numpy as jnp
from jax import lax
from jax.experimental import pallas as pl
from jax.experimental.pallas import tpu as pltpu
from jax.sharding import PartitionSpec as P


HEADS = 16
KV_HEADS = 4
HEAD_DIM = 64
BALL = 256
BLOCK = 128
CMP = 64
PICKS = 4
CAP = 2
EPS = 1e-06
LOG2E = math.log2(math.e)

ROWS = 512
PTS = 32
ZS = 4
BLK_DEV = 16
GROUP_W = 256
PAIR_W = 128
RATIO = HEADS // KV_HEADS
SUM_LOCAL = ROWS // CMP
SUM_ROWS = KV_HEADS * SUM_LOCAL
PAY_ROWS = SUM_ROWS + 16
PER = ROWS // BLOCK
BALLS = ROWS // BALL
FFN = 2048
UNIT = 256
STEPS = 2
GROUPS = ((0,), (1,), (3, 2))


bf16 = jnp.bfloat16
f32 = jnp.float32
VMEM = pltpu.VMEM
SMEM = pltpu.SMEM
NT = (((1,), (1,)), ((), ()))


def whole(space):
    return pl.BlockSpec(memory_space=space)


def near_core(array):
    return pltpu.with_memory_space_constraint(array, VMEM)


def far_core(array):
    return pltpu.with_memory_space_constraint(array, pltpu.HBM)


def params(mib):
    return pltpu.CompilerParams(vmem_limit_bytes=mib * 1024 * 1024)


def cost(flops, moved):
    return pl.CostEstimate(flops=flops, bytes_accessed=moved, transcendentals=0)


def head_ones(width):
    r = lax.broadcasted_iota(jnp.int32, (width, width), 0) // HEAD_DIM
    c = lax.broadcasted_iota(jnp.int32, (width, width), 1) // HEAD_DIM
    return jnp.where(r == c, 1.0, 0.0).astype(bf16)


def head_norm(raw, ones):
    squares = raw * raw
    high = squares.astype(bf16)
    low = (squares - high.astype(f32)).astype(bf16)
    sums = jnp.dot(high, ones, preferred_element_type=f32) + jnp.dot(
        low, ones, preferred_element_type=f32
    )
    return raw * lax.rsqrt(sums * (1.0 / HEAD_DIM) + EPS)


def row_norm(x):
    return x * lax.rsqrt(jnp.mean(x * x, axis=-1, keepdims=True) + EPS)


def first_body(
    z, picks_in, tokens_in, key_in, value_in,
    c0, c1, c2, c3, payload_out, normed_out, slots,
    table, tokens, w_key, w_value, normed, keys_held, values_held, pairs, payload, picks, sems, out_sem,
):
    rows_n = ROWS // STEPS
    weight_copies = [
        pltpu.make_async_copy(key_in, w_key, sems.at[0]),
        pltpu.make_async_copy(value_in, w_value, sems.at[1]),
    ]
    token_copies = [
        pltpu.make_async_copy(
            tokens_in.at[pl.ds(i * rows_n, rows_n)],
            tokens.at[pl.ds(i * rows_n, rows_n)],
            sems.at[2 + i],
        )
        for i in range(STEPS)
    ]
    picks_copy = pltpu.make_async_copy(picks_in, picks, out_sem.at[1])
    picks_copy.start()
    token_copies[0].start()
    weight_copies[0].start()
    weight_copies[1].start()
    for c in token_copies[1:]:
        c.start()

    def clear(i, _):
        table[i] = -1
        return 0

    lax.fori_loop(0, PTS * CAP, clear, 0, unroll=8)

    def assign(i, _):
        row = i // PICKS
        col = i % PICKS
        pick = picks[col, row]
        owner = pick // BLK_DEV
        offset = pick % BLK_DEV
        first = table[owner * CAP]
        slot = jnp.where((first == offset) | (first == -1), 0, 1)
        table[owner * CAP + slot] = offset
        slots[row, col] = owner * CAP + slot
        return 0

    picks_copy.wait()
    lax.fori_loop(0, BLK_DEV * PICKS, assign, 0, unroll=4)

    ones = head_ones(GROUP_W)
    key_means, value_means = [], []
    for i in range(STEPS):
        rows = pl.ds(i * rows_n, rows_n)
        token_copies[i].wait()
        here = row_norm(tokens[rows].astype(f32)).astype(bf16)
        normed[rows] = here
        if i == STEPS - 1:
            normed_copy = pltpu.make_async_copy(normed, normed_out, out_sem.at[2])
            normed_copy.start()
        if i == 0:
            weight_copies[0].wait()
        keys = jnp.dot(here, w_key[...], preferred_element_type=f32)
        keys = head_norm(keys, ones).astype(bf16)
        if i == 0:
            weight_copies[1].wait()
        values = jnp.dot(here, w_value[...], preferred_element_type=f32).astype(bf16)
        runs = (rows_n // CMP, CMP, GROUP_W)
        key_means.append(jnp.mean(keys.astype(f32).reshape(runs), axis=1))
        value_means.append(jnp.mean(values.astype(f32).reshape(runs), axis=1))
        keys_held[rows] = keys
        values_held[rows] = values
    summary_key = head_norm(jnp.concatenate(key_means, axis=0), ones)
    summary_value = jnp.concatenate(value_means, axis=0)
    summary = jnp.concatenate(
        [
            jnp.concatenate(
                [
                    summary_key[:, g * HEAD_DIM : (g + 1) * HEAD_DIM],
                    summary_value[:, g * HEAD_DIM : (g + 1) * HEAD_DIM],
                ],
                axis=1,
            )
            for g in range(KV_HEADS)
        ],
        axis=0,
    ).astype(bf16)
    lane = lax.broadcasted_iota(jnp.int32, (16, PAIR_W), 1)
    for o in range(PTS):
        payload[o, :SUM_ROWS, :] = summary
        first = jnp.maximum(table[o * CAP], 0)
        second = jnp.maximum(table[o * CAP + 1], 0)
        payload[o, SUM_ROWS:, :] = jnp.where(lane == 0, first, second).astype(f32).astype(bf16)
    told = pltpu.make_async_copy(payload, payload_out, out_sem.at[0])
    told.start()
    for g in range(KV_HEADS):
        lanes = slice(g * HEAD_DIM, (g + 1) * HEAD_DIM)
        pairs[g] = jnp.concatenate([keys_held[:, lanes], values_held[:, lanes]], axis=1)
    for k, c in enumerate((c0, c1, c2, c3)):
        c[...] = pairs[(z[0] + k) % ZS]
    told.wait()
    normed_copy.wait()


def first_stage(z, picks, tokens, w_key, w_value):
    hbm = whole(pltpu.HBM)
    return pl.pallas_call(
        first_body,
        name="first_stage",
        in_specs=[whole(SMEM)] + [hbm] * 4,
        out_specs=[whole(VMEM)] * ZS + [hbm, hbm, whole(SMEM)],
        out_shape=[VMEM((ROWS, PAIR_W), bf16)] * ZS
        + [
            pltpu.HBM((PTS, PAY_ROWS, PAIR_W), bf16),
            pltpu.HBM((ROWS, 1024), bf16),
            jax.ShapeDtypeStruct((BLK_DEV, PICKS), jnp.int32),
        ],
        scratch_shapes=[
            SMEM((PTS * CAP,), jnp.int32),
            VMEM((ROWS, 1024), bf16),
            VMEM((1024, GROUP_W), bf16),
            VMEM((1024, GROUP_W), bf16),
            VMEM((ROWS, 1024), bf16),
            VMEM((ROWS, GROUP_W), bf16),
            VMEM((ROWS, GROUP_W), bf16),
            VMEM((KV_HEADS, ROWS, PAIR_W), bf16),
            VMEM((PTS, PAY_ROWS, PAIR_W), bf16),
            SMEM((PICKS, BLK_DEV), jnp.int32),
            pltpu.SemaphoreType.DMA((2 + STEPS,)),
            pltpu.SemaphoreType.DMA((3,)),
        ],
        compiler_params=params(16),
        cost_estimate=cost(2 * ROWS * 1024 * 512, 4 << 20),
    )(z, *[far_core(a) for a in (picks, tokens, w_key, w_value)])


def q_body(z, normed_in, w_query, q0, q1, q2, q3, normed, raw, queries, sems):
    half = ROWS // 2
    ins = [
        pltpu.make_async_copy(
            normed_in.at[pl.ds(i * half, half)], normed.at[pl.ds(i * half, half)], sems.at[ZS + i]
        )
        for i in range(2)
    ]
    for c in ins:
        c.start()
    ones = head_ones(GROUP_W)

    def project(k, rows):
        start = pl.multiple_of(((z[0] + k) % ZS) * GROUP_W, GROUP_W)
        raw[k % 2, rows] = jnp.dot(
            normed[rows], w_query[:, pl.ds(start, GROUP_W)], preferred_element_type=f32
        )

    for i in range(2):
        ins[i].wait()
        project(0, slice(i * half, (i + 1) * half))
    outs = []
    for k, out in enumerate((q0, q1, q2, q3)):
        if k + 1 < ZS:
            project(k + 1, slice(0, ROWS))
        queries[k] = head_norm(raw[k % 2], ones).astype(bf16)
        outs.append(pltpu.make_async_copy(queries.at[k], out, sems.at[k]))
        outs[-1].start()
    for c in outs:
        c.wait()


def q_stage(z, normed, w_query):
    hbm = whole(pltpu.HBM)
    return pl.pallas_call(
        q_body,
        name="q_stage",
        in_specs=[whole(SMEM), hbm, whole(VMEM)],
        out_specs=[hbm] * ZS,
        out_shape=[pltpu.HBM((ROWS, GROUP_W), bf16)] * ZS,
        scratch_shapes=[
            VMEM((ROWS, 1024), bf16),
            VMEM((2, ROWS, GROUP_W), f32),
            VMEM((ZS, ROWS, GROUP_W), bf16),
            pltpu.SemaphoreType.DMA((ZS + 2,)),
        ],
        compiler_params=params(12),
        cost_estimate=cost(2 * ROWS * 1024 * 1024, 4 << 20),
    )(z, far_core(normed), near_core(w_query))


def reply_body(
    z, told, c0, c1, c2, c3, replies, s0, s1, s2, s3, kv_out, held, sums, asked_v, asked, sems, sum_sems
):
    asked_v[...] = told[:, SUM_ROWS, :].astype(f32).astype(jnp.int32)
    fetch = pltpu.make_async_copy(asked_v, asked, sum_sems.at[ZS])
    fetch.start()
    for k, c in enumerate((c0, c1, c2, c3)):
        held[k] = c[...].reshape(PER, BLOCK, PAIR_W)
    outs = [pltpu.make_async_copy(held, kv_out, sum_sems.at[ZS + 1])]
    fetch.wait()

    def copy(i):
        b = asked[i // CAP, i % CAP]
        k = (z[0] - b // PER + ZS) % ZS
        return pltpu.make_async_copy(held.at[k, b % PER], replies.at[i], sems.at[i])

    def start_one(i, _):
        copy(i).start()
        return 0

    def wait_one(i, _):
        copy(i).wait()
        return 0

    lax.fori_loop(0, PTS * CAP, start_one, 0, unroll=4)
    for k, s in enumerate((s0, s1, s2, s3)):
        start = pl.multiple_of(((z[0] + k) % ZS) * SUM_LOCAL, SUM_LOCAL)
        sums[k] = told[:, pl.ds(start, SUM_LOCAL), :].reshape(PTS * SUM_LOCAL, PAIR_W)
        outs.append(pltpu.make_async_copy(sums.at[k], s, sum_sems.at[k]))
    for c in outs:
        c.start()
    lax.fori_loop(0, PTS * CAP, wait_one, 0, unroll=4)
    for c in outs:
        c.wait()


def reply_stage(z, told, chunks):
    hbm = whole(pltpu.HBM)
    return pl.pallas_call(
        reply_body,
        name="reply_stage",
        in_specs=[whole(SMEM)] + [whole(VMEM)] * 5,
        out_specs=[hbm] * (ZS + 2),
        out_shape=[pltpu.HBM((PTS * CAP, BLOCK, PAIR_W), bf16)]
        + [pltpu.HBM((PTS * SUM_LOCAL, PAIR_W), bf16)] * ZS
        + [pltpu.HBM((ZS, PER, BLOCK, PAIR_W), bf16)],
        scratch_shapes=[
            VMEM((ZS, PER, BLOCK, PAIR_W), bf16),
            VMEM((ZS, PTS * SUM_LOCAL, PAIR_W), bf16),
            VMEM((PTS, PAIR_W), jnp.int32),
            SMEM((PTS, PAIR_W), jnp.int32),
            pltpu.SemaphoreType.DMA((PTS * CAP,)),
            pltpu.SemaphoreType.DMA((ZS + 2,)),
        ],
        compiler_params=params(8),
    )(z, near_core(told), *[near_core(c) for c in chunks])


def ones_beside(kv):
    return jnp.concatenate([jnp.ones((kv.shape[0], HEAD_DIM), kv.dtype), kv[:, HEAD_DIM:]], axis=1)


def near_body(chunks, z, scale, kv, s0, s1, s2, s3, *rest):
    n = len(chunks)
    qs, outs = rest[:n], rest[-6 - 2 * n : -6]
    held, q, state, peaks, sems, peak_sems = rest[-6:]
    sums = jnp.concatenate([s0[...], s1[...], s2[...], s3[...]], axis=0)
    sum_keys = sums[:, :HEAD_DIM]
    sum_values = ones_beside(sums)
    half = BALL // BLOCK

    def copies(c, b, r):
        return (
            pltpu.make_async_copy(state.at[c, b, r], outs[2 * c].at[b, r], sems.at[c, b, r]),
            pltpu.make_async_copy(peaks.at[c, b, r], outs[2 * c + 1].at[b, r], peak_sems.at[c, b, r]),
        )

    def one_chunk(c, here_of, chunk, start_copies):
        balls = [kv[chunk, pl.ds(b * half, half)].reshape(BALL, PAIR_W) for b in range(BALLS)]
        values = [ones_beside(ball) for ball in balls]
        units = [(b, r) for b in range(BALLS) for r in range(RATIO)]

        def scores(u):
            b, r = units[u]
            here = here_of(b, r)
            ball = lax.dot_general(
                here, balls[b][:, :HEAD_DIM], NT, preferred_element_type=f32
            )
            far = lax.dot_general(here, sum_keys, NT, preferred_element_type=f32)
            held[u % 2, :, :BALL] = ball
            held[u % 2, :, BALL:] = far
            peak = jnp.maximum(
                jnp.max(ball, axis=1, keepdims=True), jnp.max(far, axis=1, keepdims=True)
            )
            return peak.astype(bf16).astype(f32)

        peak = scores(0)
        for u, (b, r) in enumerate(units):
            coming = scores(u + 1) if u + 1 < len(units) else None
            factor = scale[z[0] * RATIO + r] * (LOG2E / math.sqrt(HEAD_DIM))
            w = jnp.exp2((held[u % 2] - peak) * factor).astype(bf16)
            peaks[c, b, r] = jnp.broadcast_to(peak, (BALL, PAIR_W)).astype(bf16)
            state[c, b, r] = jnp.dot(w[:, :BALL], values[b], preferred_element_type=f32) + jnp.dot(
                w[:, BALL:], sum_values, preferred_element_type=f32
            )
            start_copies(b, r)
            peak = coming

    def part(ref):
        def take(b, r):
            return ref[b * BALL : (b + 1) * BALL, r * HEAD_DIM : (r + 1) * HEAD_DIM]

        return take

    if n == 1:

        def begin(b, r):
            for c in copies(0, b, r):
                c.start()

        one_chunk(0, part(qs[0]), chunks[0], begin)
    else:

        def loop(c, _):
            for i in range(n):

                @pl.when(c == i)
                def _():
                    q[...] = qs[i][...]

            chunk = jnp.where(c == 0, chunks[0], chunks[1])
            one_chunk(c, part(q), chunk, lambda b, r: None)
            for i in range(n):

                @pl.when(c == i)
                def _():
                    for b in range(BALLS):
                        for r in range(RATIO):
                            for m in copies(i, b, r):
                                m.start()

            return 0

        lax.fori_loop(0, n, loop, 0)
    for c in range(n):
        for b in range(BALLS):
            for r in range(RATIO):
                for m in copies(c, b, r):
                    m.wait()


def near_stage(chunks, z, scale, qs, kv, sums, others):
    n = len(chunks)
    shape = (BALLS, RATIO, BALL, PAIR_W)
    outs = pl.pallas_call(
        functools.partial(near_body, chunks),
        name="near_stage",
        in_specs=[whole(SMEM)] * 2 + [whole(VMEM)] * (5 + n) + [whole(pl.ANY)] * len(others),
        out_specs=[whole(pltpu.HBM)] * (2 * n),
        out_shape=[pltpu.HBM(shape, f32), pltpu.HBM(shape, bf16)] * n,
        scratch_shapes=[
            VMEM((2, BALL, BALL + PTS * SUM_LOCAL * ZS), f32),
            VMEM((ROWS if n > 1 else 16, GROUP_W), bf16),
            VMEM((n, *shape), f32),
            VMEM((n, *shape), bf16),
            pltpu.SemaphoreType.DMA((n, BALLS, RATIO)),
            pltpu.SemaphoreType.DMA((n, BALLS, RATIO)),
        ],
        compiler_params=params(14),
        cost_estimate=cost(8 * 4 * n * ROWS * 1280 * 64, 2 << 20),
    )(
        z,
        scale,
        near_core(kv),
        *[near_core(s) for s in sums],
        *[near_core(q) for q in qs],
        *[far_core(a) for a in others],
    )
    return [outs[2 * c : 2 * c + 2] for c in range(n)]


def far_body(shift_by, direct, z, slots, scale, q, state, peaks, fetched, *rest):
    if direct:
        out, held, state_held, peaks_held, sems = rest[-5:]
        brought = []
        for b in range(BALLS):
            brought.append(
                (
                    pltpu.make_async_copy(state.at[b], state_held.at[b], sems.at[b, 0]),
                    pltpu.make_async_copy(peaks.at[b], peaks_held.at[b], sems.at[b, 1]),
                )
            )
            for c in brought[-1]:
                c.start()
        state, peaks = state_held, peaks_held
    else:
        out, held = rest[-2:]
    lane = lax.broadcasted_iota(jnp.int32, (BLOCK, PAIR_W), 1)
    first_row = ((z[0] - shift_by + ZS) % ZS) * PER

    def part(r):
        return slice(r * BLOCK, (r + 1) * BLOCK)

    def keys_of(i):
        return jnp.concatenate([fetched[slots[first_row + i, j]] for j in range(PICKS)], axis=0)

    def scores(i, slot):
        here = jnp.concatenate(
            [q[pl.ds(i * BLOCK, BLOCK), r * HEAD_DIM : (r + 1) * HEAD_DIM] for r in range(RATIO)],
            axis=0,
        )
        s = lax.dot_general(here, keys_of(i)[:, :HEAD_DIM], NT, preferred_element_type=f32)
        held[slot] = s
        return jnp.max(s, axis=1, keepdims=True)

    def finish(b, i, slot, peak):
        rows = slice(slot * BLOCK, (slot + 1) * BLOCK)
        weights, keeps = [], []
        for r in range(RATIO):
            factor = scale[z[0] * RATIO + r] * (LOG2E / math.sqrt(HEAD_DIM))
            before = peaks[b, r, rows, :].astype(f32)
            new = jnp.maximum(before, peak[part(r)])
            s = held[slot, part(r), :]
            weights.append(
                jnp.concatenate(
                    [
                        jnp.exp2((s[:, part(j)] - new) * factor).astype(bf16)
                        for j in range(PICKS)
                    ],
                    axis=1,
                )
            )
            keeps.append(jnp.exp2((before - new) * factor))
        o = jnp.dot(
            jnp.concatenate(weights, axis=0), ones_beside(keys_of(i)), preferred_element_type=f32
        )
        for r in range(0, RATIO, 2):
            even = state[b, r, rows, :] * keeps[r] + o[part(r)]
            odd = state[b, r + 1, rows, :] * keeps[r + 1] + o[part(r + 1)]
            total = jnp.where(lane < HEAD_DIM, even, pltpu.roll(odd, HEAD_DIM, 1))
            summed = jnp.where(lane < HEAD_DIM, pltpu.roll(even, HEAD_DIM, 1), odd)
            out[pl.ds(i * BLOCK, BLOCK), r * HEAD_DIM : (r + 2) * HEAD_DIM] = (
                summed / total
            ).astype(bf16)

    def one_ball(b, peak):
        coming = scores(2 * b + 1, 1)
        finish(b, 2 * b, 0, peak)
        after = scores(2 * b + 2, 0) if b + 1 < BALLS else None
        if direct and b + 1 < BALLS:
            for c in brought[b + 1]:
                c.wait()
        finish(b, 2 * b + 1, 1, coming)
        return after

    peak = scores(0, 0)
    if direct:
        for c in brought[0]:
            c.wait()
    for b in range(BALLS):
        peak = one_ball(b, peak)


def far_stage(shift_by, z, slots, scale, q, state, fetched, others, direct=False):
    shape = (BALLS, RATIO, BALL, PAIR_W)
    place, keep = (pltpu.HBM, far_core) if direct else (VMEM, near_core)
    extra = [VMEM(shape, f32), VMEM(shape, bf16), pltpu.SemaphoreType.DMA((BALLS, 2))]
    return pl.pallas_call(
        functools.partial(far_body, shift_by, direct),
        name="far_stage",
        in_specs=[whole(SMEM)] * 3
        + [whole(VMEM)]
        + [whole(place)] * 2
        + [whole(VMEM)]
        + [whole(pl.ANY)] * len(others),
        out_specs=whole(VMEM),
        out_shape=VMEM((ROWS, GROUP_W), bf16),
        scratch_shapes=[VMEM((2, RATIO * BLOCK, PICKS * BLOCK), f32)] + (extra if direct else []),
        compiler_params=params(12),
        cost_estimate=cost(8 * 4 * ROWS * 512 * 64, 4 << 20),
    )(
        z,
        slots,
        scale,
        near_core(q),
        *[keep(a) for a in state],
        near_core(fetched),
        *[far_core(a) for a in others],
    )


def ffn_body(z, tokens, a0, a1, a2, a3, w_out, w_gate, w_up, w_down, out, mid_held, held, hidden):
    mid = tokens[...].astype(f32)
    for k, a in enumerate((a0, a1, a2, a3)):
        start = pl.multiple_of(((z[0] + k) % ZS) * GROUP_W, GROUP_W)
        mid = mid + jnp.dot(a[...], w_out[pl.ds(start, GROUP_W), :], preferred_element_type=f32)
    mid_held[...] = mid
    held[...] = row_norm(mid).astype(bf16)
    for j in range(FFN // UNIT):
        cols = slice(j * UNIT, (j + 1) * UNIT)
        gate = jnp.dot(held[...], w_gate[:, cols], preferred_element_type=f32)
        upward = jnp.dot(held[...], w_up[:, cols], preferred_element_type=f32)
        hidden[:, cols] = (gate / (1.0 + jnp.exp(-gate)) * upward).astype(bf16)
    out[...] = (
        mid_held[...] + jnp.dot(hidden[...], w_down[...], preferred_element_type=f32)
    ).astype(bf16)


def ffn_stage(z, tokens, parts, w_out, w_gate, w_up, w_down):
    return pl.pallas_call(
        ffn_body,
        name="ffn_stage",
        in_specs=[whole(SMEM)] + [whole(VMEM)] * 9,
        out_specs=whole(VMEM),
        out_shape=jax.ShapeDtypeStruct((ROWS, 1024), bf16),
        scratch_shapes=[VMEM((ROWS, 1024), f32), VMEM((ROWS, 1024), bf16), VMEM((ROWS, FFN), bf16)],
        compiler_params=params(14),
        cost_estimate=cost(2 * ROWS * 1024 * 7168, 18 << 20),
    )(z, *[near_core(a) for a in (tokens, *parts, w_out, w_gate, w_up, w_down)])


def shift(array, k):
    return lax.ppermute(array, "head", [(i, (i + k) % ZS) for i in range(ZS)])


def body(tokens, w_query, w_key, w_value, w_out, logit_scale, w_gate, w_up, w_down, picks):
    z = lax.axis_index("head").astype(jnp.int32).reshape(1)
    *pairs, payload, normed, slots = first_stage(z, picks.T, tokens, w_key, w_value)
    chunks = [pairs[0]] + [shift(pairs[k], k) for k in (1, 2, 3)]
    told = lax.all_to_all(payload, "pts", split_axis=0, concat_axis=0, tiled=True)
    query = q_stage(z, normed, w_query)
    replies, *sums, kv = reply_stage(z, told, chunks)
    replies = replies.reshape(PTS, CAP * BLOCK, PAIR_W)
    fetched = lax.all_to_all(replies, "pts", split_axis=0, concat_axis=0, tiled=True)
    fetched = fetched.reshape(PTS * CAP, BLOCK, PAIR_W)
    sums = [sums[0]] + [shift(sums[k], k) for k in (1, 2, 3)]
    q = [query[0], None, None, None]
    for k in (1, 3, 2):
        q[k] = shift(query[k], k)
    states = [None] * ZS
    done = []
    for group in GROUPS:
        made = near_stage(group, z, logit_scale, [q[k] for k in group], kv, sums, done)
        for k, one in zip(group, made):
            states[k] = one
        done = made[-1]
    parts = [None] * ZS
    for k in (2, 1, 3, 0):
        others = states[2] if k != 2 else []
        attended = far_stage(k, z, slots, logit_scale, q[k], states[k], fetched, others, k == 2)
        parts[k] = shift(attended, ZS - k) if k else attended
    return ffn_stage(z, tokens, parts, w_out, w_gate, w_up, w_down)


def solution(mesh):
    placed = (P(("pts", "head"), None), P(), P(), P(), P(), P(), P(), P(), P(), P("pts", None))
    return jax.shard_map(
        body, mesh=mesh, in_specs=placed, out_specs=P(("pts", "head"), None), check_vma=False
    )
```

```python
import functools
import math

import jax
import jax.numpy as jnp
from jax import lax
from jax.experimental import pallas as pl
from jax.experimental.pallas import tpu as pltpu
from jax.sharding import PartitionSpec as P


HEADS = 16
KV_HEADS = 4
HEAD_DIM = 64
BALL = 256
BLOCK = 128
CMP = 64
PICKS = 4
CAP = 2
EPS = 1e-06
LOG2E = math.log2(math.e)

ROWS = 512
PTS = 32
ZS = 4
BLK_DEV = 16
GROUP_W = 256
PAIR_W = 128
RATIO = HEADS // KV_HEADS
SUM_LOCAL = ROWS // CMP
SUM_ROWS = KV_HEADS * SUM_LOCAL
PAY_ROWS = SUM_ROWS + 16
PER = ROWS // BLOCK
BALLS = ROWS // BALL
FFN = 2048
UNIT = 256
STEPS = 2
GROUPS = ((0,), (1,), (3, 2))


bf16 = jnp.bfloat16
f32 = jnp.float32
VMEM = pltpu.VMEM
SMEM = pltpu.SMEM
NT = (((1,), (1,)), ((), ()))


def whole(space):
    return pl.BlockSpec(memory_space=space)


def near_core(array):
    return pltpu.with_memory_space_constraint(array, VMEM)


def far_core(array):
    return pltpu.with_memory_space_constraint(array, pltpu.HBM)


def params(mib):
    return pltpu.CompilerParams(vmem_limit_bytes=mib * 1024 * 1024)


def cost(flops, moved):
    return pl.CostEstimate(flops=flops, bytes_accessed=moved, transcendentals=0)


def head_ones(width):
    r = lax.broadcasted_iota(jnp.int32, (width, width), 0) // HEAD_DIM
    c = lax.broadcasted_iota(jnp.int32, (width, width), 1) // HEAD_DIM
    return jnp.where(r == c, 1.0, 0.0).astype(bf16)


def head_norm(raw, ones):
    squares = raw * raw
    high = squares.astype(bf16)
    low = (squares - high.astype(f32)).astype(bf16)
    sums = jnp.dot(high, ones, preferred_element_type=f32) + jnp.dot(
        low, ones, preferred_element_type=f32
    )
    return raw * lax.rsqrt(sums * (1.0 / HEAD_DIM) + EPS)


def row_norm(x):
    return x * lax.rsqrt(jnp.mean(x * x, axis=-1, keepdims=True) + EPS)


def first_body(
    z, picks_in, tokens_in, key_in, value_in,
    c0, c1, c2, c3, payload_out, normed_out, slots,
    table, tokens, w_key, w_value, normed, keys_held, values_held, pairs, payload, picks, sems, out_sem,
):
    rows_n = ROWS // STEPS
    weight_copies = [
        pltpu.make_async_copy(key_in, w_key, sems.at[0]),
        pltpu.make_async_copy(value_in, w_value, sems.at[1]),
    ]
    token_copies = [
        pltpu.make_async_copy(
            tokens_in.at[pl.ds(i * rows_n, rows_n)],
            tokens.at[pl.ds(i * rows_n, rows_n)],
            sems.at[2 + i],
        )
        for i in range(STEPS)
    ]
    picks_copy = pltpu.make_async_copy(picks_in, picks, out_sem.at[1])
    picks_copy.start()
    token_copies[0].start()
    weight_copies[0].start()
    weight_copies[1].start()
    for c in token_copies[1:]:
        c.start()

    def clear(i, _):
        table[i] = -1
        return 0

    lax.fori_loop(0, PTS * CAP, clear, 0, unroll=8)

    def assign(i, _):
        row = i // PICKS
        col = i % PICKS
        pick = picks[col, row]
        owner = pick // BLK_DEV
        offset = pick % BLK_DEV
        first = table[owner * CAP]
        slot = jnp.where((first == offset) | (first == -1), 0, 1)
        table[owner * CAP + slot] = offset
        slots[row, col] = owner * CAP + slot
        return 0

    picks_copy.wait()
    lax.fori_loop(0, BLK_DEV * PICKS, assign, 0, unroll=4)

    ones = head_ones(GROUP_W)
    key_means, value_means = [], []
    for i in range(STEPS):
        rows = pl.ds(i * rows_n, rows_n)
        token_copies[i].wait()
        here = row_norm(tokens[rows].astype(f32)).astype(bf16)
        normed[rows] = here
        if i == STEPS - 1:
            normed_copy = pltpu.make_async_copy(normed, normed_out, out_sem.at[2])
            normed_copy.start()
        if i == 0:
            weight_copies[0].wait()
        keys = jnp.dot(here, w_key[...], preferred_element_type=f32)
        keys = head_norm(keys, ones).astype(bf16)
        if i == 0:
            weight_copies[1].wait()
        values = jnp.dot(here, w_value[...], preferred_element_type=f32).astype(bf16)
        runs = (rows_n // CMP, CMP, GROUP_W)
        key_means.append(jnp.mean(keys.astype(f32).reshape(runs), axis=1))
        value_means.append(jnp.mean(values.astype(f32).reshape(runs), axis=1))
        keys_held[rows] = keys
        values_held[rows] = values
    summary_key = head_norm(jnp.concatenate(key_means, axis=0), ones)
    summary_value = jnp.concatenate(value_means, axis=0)
    summary = jnp.concatenate(
        [
            jnp.concatenate(
                [
                    summary_key[:, g * HEAD_DIM : (g + 1) * HEAD_DIM],
                    summary_value[:, g * HEAD_DIM : (g + 1) * HEAD_DIM],
                ],
                axis=1,
            )
            for g in range(KV_HEADS)
        ],
        axis=0,
    ).astype(bf16)
    lane = lax.broadcasted_iota(jnp.int32, (16, PAIR_W), 1)
    for o in range(PTS):
        payload[o, :SUM_ROWS, :] = summary
        first = jnp.maximum(table[o * CAP], 0)
        second = jnp.maximum(table[o * CAP + 1], 0)
        payload[o, SUM_ROWS:, :] = jnp.where(lane == 0, first, second).astype(f32).astype(bf16)
    told = pltpu.make_async_copy(payload, payload_out, out_sem.at[0])
    told.start()
    for g in range(KV_HEADS):
        lanes = slice(g * HEAD_DIM, (g + 1) * HEAD_DIM)
        pairs[g] = jnp.concatenate([keys_held[:, lanes], values_held[:, lanes]], axis=1)
    for k, c in enumerate((c0, c1, c2, c3)):
        c[...] = pairs[(z[0] + k) % ZS]
    told.wait()
    normed_copy.wait()


def first_stage(z, picks, tokens, w_key, w_value):
    hbm = whole(pltpu.HBM)
    return pl.pallas_call(
        first_body,
        name="first_stage",
        in_specs=[whole(SMEM)] + [hbm] * 4,
        out_specs=[whole(VMEM)] * ZS + [hbm, hbm, whole(SMEM)],
        out_shape=[VMEM((ROWS, PAIR_W), bf16)] * ZS
        + [
            pltpu.HBM((PTS, PAY_ROWS, PAIR_W), bf16),
            pltpu.HBM((ROWS, 1024), bf16),
            jax.ShapeDtypeStruct((BLK_DEV, PICKS), jnp.int32),
        ],
        scratch_shapes=[
            SMEM((PTS * CAP,), jnp.int32),
            VMEM((ROWS, 1024), bf16),
            VMEM((1024, GROUP_W), bf16),
            VMEM((1024, GROUP_W), bf16),
            VMEM((ROWS, 1024), bf16),
            VMEM((ROWS, GROUP_W), bf16),
            VMEM((ROWS, GROUP_W), bf16),
            VMEM((KV_HEADS, ROWS, PAIR_W), bf16),
            VMEM((PTS, PAY_ROWS, PAIR_W), bf16),
            SMEM((PICKS, BLK_DEV), jnp.int32),
            pltpu.SemaphoreType.DMA((2 + STEPS,)),
            pltpu.SemaphoreType.DMA((3,)),
        ],
        compiler_params=params(16),
        cost_estimate=cost(2 * ROWS * 1024 * 512, 4 << 20),
    )(z, *[far_core(a) for a in (picks, tokens, w_key, w_value)])


def q_body(z, normed_in, w_query, q0, q1, q2, q3, normed, raw, queries, sems):
    half = ROWS // 2
    ins = [
        pltpu.make_async_copy(
            normed_in.at[pl.ds(i * half, half)], normed.at[pl.ds(i * half, half)], sems.at[ZS + i]
        )
        for i in range(2)
    ]
    for c in ins:
        c.start()
    ones = head_ones(GROUP_W)

    def project(k, rows):
        start = pl.multiple_of(((z[0] + k) % ZS) * GROUP_W, GROUP_W)
        raw[k % 2, rows] = jnp.dot(
            normed[rows], w_query[:, pl.ds(start, GROUP_W)], preferred_element_type=f32
        )

    for i in range(2):
        ins[i].wait()
        project(0, slice(i * half, (i + 1) * half))
    outs = []
    for k, out in enumerate((q0, q1, q2, q3)):
        if k + 1 < ZS:
            project(k + 1, slice(0, ROWS))
        queries[k] = head_norm(raw[k % 2], ones).astype(bf16)
        outs.append(pltpu.make_async_copy(queries.at[k], out, sems.at[k]))
        outs[-1].start()
    for c in outs:
        c.wait()


def q_stage(z, normed, w_query):
    hbm = whole(pltpu.HBM)
    return pl.pallas_call(
        q_body,
        name="q_stage",
        in_specs=[whole(SMEM), hbm, whole(VMEM)],
        out_specs=[hbm] * ZS,
        out_shape=[pltpu.HBM((ROWS, GROUP_W), bf16)] * ZS,
        scratch_shapes=[
            VMEM((ROWS, 1024), bf16),
            VMEM((2, ROWS, GROUP_W), f32),
            VMEM((ZS, ROWS, GROUP_W), bf16),
            pltpu.SemaphoreType.DMA((ZS + 2,)),
        ],
        compiler_params=params(12),
        cost_estimate=cost(2 * ROWS * 1024 * 1024, 4 << 20),
    )(z, far_core(normed), near_core(w_query))


def reply_body(
    z, told, c0, c1, c2, c3, replies, s0, s1, s2, s3, kv_out, held, sums, asked_v, asked, sems, sum_sems
):
    asked_v[...] = told[:, SUM_ROWS, :].astype(f32).astype(jnp.int32)
    fetch = pltpu.make_async_copy(asked_v, asked, sum_sems.at[ZS])
    fetch.start()
    for k, c in enumerate((c0, c1, c2, c3)):
        held[k] = c[...].reshape(PER, BLOCK, PAIR_W)
    outs = [pltpu.make_async_copy(held, kv_out, sum_sems.at[ZS + 1])]
    fetch.wait()

    def copy(i):
        b = asked[i // CAP, i % CAP]
        k = (z[0] - b // PER + ZS) % ZS
        return pltpu.make_async_copy(held.at[k, b % PER], replies.at[i], sems.at[i])

    def start_one(i, _):
        copy(i).start()
        return 0

    def wait_one(i, _):
        copy(i).wait()
        return 0

    lax.fori_loop(0, PTS * CAP, start_one, 0, unroll=4)
    for k, s in enumerate((s0, s1, s2, s3)):
        start = pl.multiple_of(((z[0] + k) % ZS) * SUM_LOCAL, SUM_LOCAL)
        sums[k] = told[:, pl.ds(start, SUM_LOCAL), :].reshape(PTS * SUM_LOCAL, PAIR_W)
        outs.append(pltpu.make_async_copy(sums.at[k], s, sum_sems.at[k]))
    for c in outs:
        c.start()
    lax.fori_loop(0, PTS * CAP, wait_one, 0, unroll=4)
    for c in outs:
        c.wait()


def reply_stage(z, told, chunks):
    hbm = whole(pltpu.HBM)
    return pl.pallas_call(
        reply_body,
        name="reply_stage",
        in_specs=[whole(SMEM)] + [whole(VMEM)] * 5,
        out_specs=[hbm] * (ZS + 2),
        out_shape=[pltpu.HBM((PTS * CAP, BLOCK, PAIR_W), bf16)]
        + [pltpu.HBM((PTS * SUM_LOCAL, PAIR_W), bf16)] * ZS
        + [pltpu.HBM((ZS, PER, BLOCK, PAIR_W), bf16)],
        scratch_shapes=[
            VMEM((ZS, PER, BLOCK, PAIR_W), bf16),
            VMEM((ZS, PTS * SUM_LOCAL, PAIR_W), bf16),
            VMEM((PTS, PAIR_W), jnp.int32),
            SMEM((PTS, PAIR_W), jnp.int32),
            pltpu.SemaphoreType.DMA((PTS * CAP,)),
            pltpu.SemaphoreType.DMA((ZS + 2,)),
        ],
        compiler_params=params(8),
    )(z, near_core(told), *[near_core(c) for c in chunks])


def ones_beside(kv):
    return jnp.concatenate([jnp.ones((kv.shape[0], HEAD_DIM), kv.dtype), kv[:, HEAD_DIM:]], axis=1)


def near_body(chunks, z, scale, kv, s0, s1, s2, s3, *rest):
    n = len(chunks)
    qs, outs = rest[:n], rest[-6 - 2 * n : -6]
    held, q, state, peaks, sems, peak_sems = rest[-6:]
    sums = jnp.concatenate([s0[...], s1[...], s2[...], s3[...]], axis=0)
    sum_keys = sums[:, :HEAD_DIM]
    sum_values = ones_beside(sums)
    half = BALL // BLOCK

    def copies(c, b, r):
        return (
            pltpu.make_async_copy(state.at[c, b, r], outs[2 * c].at[b, r], sems.at[c, b, r]),
            pltpu.make_async_copy(peaks.at[c, b, r], outs[2 * c + 1].at[b, r], peak_sems.at[c, b, r]),
        )

    def one_chunk(c, here_of, chunk, start_copies):
        balls = [kv[chunk, pl.ds(b * half, half)].reshape(BALL, PAIR_W) for b in range(BALLS)]
        values = [ones_beside(ball) for ball in balls]
        units = [(b, r) for b in range(BALLS) for r in range(RATIO)]

        def scores(u):
            b, r = units[u]
            here = here_of(b, r)
            ball = lax.dot_general(
                here, balls[b][:, :HEAD_DIM], NT, preferred_element_type=f32
            )
            far = lax.dot_general(here, sum_keys, NT, preferred_element_type=f32)
            held[u % 2, :, :BALL] = ball
            held[u % 2, :, BALL:] = far
            peak = jnp.maximum(
                jnp.max(ball, axis=1, keepdims=True), jnp.max(far, axis=1, keepdims=True)
            )
            return peak.astype(bf16).astype(f32)

        peak = scores(0)
        for u, (b, r) in enumerate(units):
            coming = scores(u + 1) if u + 1 < len(units) else None
            factor = scale[z[0] * RATIO + r] * (LOG2E / math.sqrt(HEAD_DIM))
            w = jnp.exp2((held[u % 2] - peak) * factor).astype(bf16)
            peaks[c, b, r] = jnp.broadcast_to(peak, (BALL, PAIR_W)).astype(bf16)
            state[c, b, r] = jnp.dot(w[:, :BALL], values[b], preferred_element_type=f32) + jnp.dot(
                w[:, BALL:], sum_values, preferred_element_type=f32
            )
            start_copies(b, r)
            peak = coming

    def part(ref):
        def take(b, r):
            return ref[b * BALL : (b + 1) * BALL, r * HEAD_DIM : (r + 1) * HEAD_DIM]

        return take

    if n == 1:

        def begin(b, r):
            for c in copies(0, b, r):
                c.start()

        one_chunk(0, part(qs[0]), chunks[0], begin)
    else:

        def loop(c, _):
            for i in range(n):

                @pl.when(c == i)
                def _():
                    q[...] = qs[i][...]

            chunk = jnp.where(c == 0, chunks[0], chunks[1])
            one_chunk(c, part(q), chunk, lambda b, r: None)
            for i in range(n):

                @pl.when(c == i)
                def _():
                    for b in range(BALLS):
                        for r in range(RATIO):
                            for m in copies(i, b, r):
                                m.start()

            return 0

        lax.fori_loop(0, n, loop, 0)
    for c in range(n):
        for b in range(BALLS):
            for r in range(RATIO):
                for m in copies(c, b, r):
                    m.wait()


def near_stage(chunks, z, scale, qs, kv, sums, others):
    n = len(chunks)
    shape = (BALLS, RATIO, BALL, PAIR_W)
    outs = pl.pallas_call(
        functools.partial(near_body, chunks),
        name="near_stage",
        in_specs=[whole(SMEM)] * 2 + [whole(VMEM)] * (5 + n) + [whole(pl.ANY)] * len(others),
        out_specs=[whole(pltpu.HBM)] * (2 * n),
        out_shape=[pltpu.HBM(shape, f32), pltpu.HBM(shape, bf16)] * n,
        scratch_shapes=[
            VMEM((2, BALL, BALL + PTS * SUM_LOCAL * ZS), f32),
            VMEM((ROWS if n > 1 else 16, GROUP_W), bf16),
            VMEM((n, *shape), f32),
            VMEM((n, *shape), bf16),
            pltpu.SemaphoreType.DMA((n, BALLS, RATIO)),
            pltpu.SemaphoreType.DMA((n, BALLS, RATIO)),
        ],
        compiler_params=params(14),
        cost_estimate=cost(8 * 4 * n * ROWS * 1280 * 64, 2 << 20),
    )(
        z,
        scale,
        near_core(kv),
        *[near_core(s) for s in sums],
        *[near_core(q) for q in qs],
        *[far_core(a) for a in others],
    )
    return [outs[2 * c : 2 * c + 2] for c in range(n)]


def far_body(shift_by, direct, z, slots, scale, q, state, peaks, fetched, *rest):
    if direct:
        out, held, state_held, peaks_held, sems = rest[-5:]
        brought = []
        for b in range(BALLS):
            brought.append(
                (
                    pltpu.make_async_copy(state.at[b], state_held.at[b], sems.at[b, 0]),
                    pltpu.make_async_copy(peaks.at[b], peaks_held.at[b], sems.at[b, 1]),
                )
            )
            for c in brought[-1]:
                c.start()
        state, peaks = state_held, peaks_held
    else:
        out, held = rest[-2:]
    lane = lax.broadcasted_iota(jnp.int32, (BLOCK, PAIR_W), 1)
    first_row = ((z[0] - shift_by + ZS) % ZS) * PER

    def part(r):
        return slice(r * BLOCK, (r + 1) * BLOCK)

    def keys_of(i):
        return jnp.concatenate([fetched[slots[first_row + i, j]] for j in range(PICKS)], axis=0)

    def scores(i, slot):
        here = jnp.concatenate(
            [q[pl.ds(i * BLOCK, BLOCK), r * HEAD_DIM : (r + 1) * HEAD_DIM] for r in range(RATIO)],
            axis=0,
        )
        s = lax.dot_general(here, keys_of(i)[:, :HEAD_DIM], NT, preferred_element_type=f32)
        held[slot] = s
        return jnp.max(s, axis=1, keepdims=True)

    def finish(b, i, slot, peak):
        rows = slice(slot * BLOCK, (slot + 1) * BLOCK)
        weights, keeps = [], []
        for r in range(RATIO):
            factor = scale[z[0] * RATIO + r] * (LOG2E / math.sqrt(HEAD_DIM))
            before = peaks[b, r, rows, :].astype(f32)
            new = jnp.maximum(before, peak[part(r)])
            s = held[slot, part(r), :]
            weights.append(
                jnp.concatenate(
                    [
                        jnp.exp2((s[:, part(j)] - new) * factor).astype(bf16)
                        for j in range(PICKS)
                    ],
                    axis=1,
                )
            )
            keeps.append(jnp.exp2((before - new) * factor))
        o = jnp.dot(
            jnp.concatenate(weights, axis=0), ones_beside(keys_of(i)), preferred_element_type=f32
        )
        for r in range(0, RATIO, 2):
            even = state[b, r, rows, :] * keeps[r] + o[part(r)]
            odd = state[b, r + 1, rows, :] * keeps[r + 1] + o[part(r + 1)]
            total = jnp.where(lane < HEAD_DIM, even, pltpu.roll(odd, HEAD_DIM, 1))
            summed = jnp.where(lane < HEAD_DIM, pltpu.roll(even, HEAD_DIM, 1), odd)
            out[pl.ds(i * BLOCK, BLOCK), r * HEAD_DIM : (r + 2) * HEAD_DIM] = (
                summed / total
            ).astype(bf16)

    def one_ball(b, peak):
        coming = scores(2 * b + 1, 1)
        finish(b, 2 * b, 0, peak)
        after = scores(2 * b + 2, 0) if b + 1 < BALLS else None
        if direct and b + 1 < BALLS:
            for c in brought[b + 1]:
                c.wait()
        finish(b, 2 * b + 1, 1, coming)
        return after

    peak = scores(0, 0)
    if direct:
        for c in brought[0]:
            c.wait()
    for b in range(BALLS):
        peak = one_ball(b, peak)


def far_stage(shift_by, z, slots, scale, q, state, fetched, others, direct=False):
    shape = (BALLS, RATIO, BALL, PAIR_W)
    place, keep = (pltpu.HBM, far_core) if direct else (VMEM, near_core)
    extra = [VMEM(shape, f32), VMEM(shape, bf16), pltpu.SemaphoreType.DMA((BALLS, 2))]
    return pl.pallas_call(
        functools.partial(far_body, shift_by, direct),
        name="far_stage",
        in_specs=[whole(SMEM)] * 3
        + [whole(VMEM)]
        + [whole(place)] * 2
        + [whole(VMEM)]
        + [whole(pl.ANY)] * len(others),
        out_specs=whole(VMEM),
        out_shape=VMEM((ROWS, GROUP_W), bf16),
        scratch_shapes=[VMEM((2, RATIO * BLOCK, PICKS * BLOCK), f32)] + (extra if direct else []),
        compiler_params=params(12),
        cost_estimate=cost(8 * 4 * ROWS * 512 * 64, 4 << 20),
    )(
        z,
        slots,
        scale,
        near_core(q),
        *[keep(a) for a in state],
        near_core(fetched),
        *[far_core(a) for a in others],
    )


def projected(z, k, part, w_out):
    start = pl.multiple_of(((z[0] + k) % ZS) * GROUP_W, GROUP_W)
    return jnp.dot(part[...], w_out[pl.ds(start, GROUP_W), :], preferred_element_type=f32)


def mid_body(z, tokens, a0, a1, a2, w_out, out):
    mid = tokens[...].astype(f32)
    for k, a in enumerate((a0, a1, a2)):
        mid = mid + projected(z, k, a, w_out)
    out[...] = mid


def mid_stage(z, tokens, parts, w_out):
    return pl.pallas_call(
        mid_body,
        name="mid_stage",
        in_specs=[whole(SMEM)] + [whole(VMEM)] * 5,
        out_specs=whole(VMEM),
        out_shape=VMEM((ROWS, 1024), f32),
        compiler_params=params(8),
        cost_estimate=cost(2 * ROWS * 1024 * 768, 4 << 20),
    )(z, *[near_core(a) for a in (tokens, *parts, w_out)])


def ffn_body(z, mid_in, a3, w_out, w_gate, w_up, w_down, out, mid_held, held, hidden):
    mid = mid_in[...] + projected(z, 3, a3, w_out)
    mid_held[...] = mid
    held[...] = row_norm(mid).astype(bf16)
    for j in range(FFN // UNIT):
        cols = slice(j * UNIT, (j + 1) * UNIT)
        gate = jnp.dot(held[...], w_gate[:, cols], preferred_element_type=f32)
        upward = jnp.dot(held[...], w_up[:, cols], preferred_element_type=f32)
        hidden[:, cols] = (gate / (1.0 + jnp.exp(-gate)) * upward).astype(bf16)
    out[...] = (
        mid_held[...] + jnp.dot(hidden[...], w_down[...], preferred_element_type=f32)
    ).astype(bf16)


def ffn_stage(z, mid, part, w_out, w_gate, w_up, w_down):
    return pl.pallas_call(
        ffn_body,
        name="ffn_stage",
        in_specs=[whole(SMEM)] + [whole(VMEM)] * 6,
        out_specs=whole(VMEM),
        out_shape=jax.ShapeDtypeStruct((ROWS, 1024), bf16),
        scratch_shapes=[VMEM((ROWS, 1024), f32), VMEM((ROWS, 1024), bf16), VMEM((ROWS, FFN), bf16)],
        compiler_params=params(14),
        cost_estimate=cost(2 * ROWS * 1024 * 6400, 18 << 20),
    )(z, *[near_core(a) for a in (mid, part, w_out, w_gate, w_up, w_down)])


def shift(array, k):
    return lax.ppermute(array, "head", [(i, (i + k) % ZS) for i in range(ZS)])


def body(tokens, w_query, w_key, w_value, w_out, logit_scale, w_gate, w_up, w_down, picks):
    z = lax.axis_index("head").astype(jnp.int32).reshape(1)
    *pairs, payload, normed, slots = first_stage(z, picks.T, tokens, w_key, w_value)
    chunks = [pairs[0], None, None, None]
    for k in (2, 1, 3):
        chunks[k] = shift(pairs[k], k)
    told = lax.all_to_all(payload, "pts", split_axis=0, concat_axis=0, tiled=True)
    query = q_stage(z, normed, w_query)
    replies, *sums, kv = reply_stage(z, told, chunks)
    replies = replies.reshape(PTS, CAP * BLOCK, PAIR_W)
    fetched = lax.all_to_all(replies, "pts", split_axis=0, concat_axis=0, tiled=True)
    fetched = fetched.reshape(PTS * CAP, BLOCK, PAIR_W)
    sums = [sums[0]] + [shift(sums[k], k) for k in (1, 2, 3)]
    q = [query[0], None, None, None]
    for k in (1, 3, 2):
        q[k] = shift(query[k], k)
    states = [None] * ZS
    done = []
    for group in GROUPS:
        made = near_stage(group, z, logit_scale, [q[k] for k in group], kv, sums, done)
        for k, one in zip(group, made):
            states[k] = one
        done = made[-1]
    parts = [None] * ZS
    for k in (2, 1, 3, 0):
        others = states[2] if k != 2 else []
        attended = far_stage(k, z, slots, logit_scale, q[k], states[k], fetched, others, k == 2)
        parts[k] = shift(attended, ZS - k) if k else attended
    mid = mid_stage(z, tokens, parts[:3], w_out)
    return ffn_stage(z, mid, parts[3], w_out, w_gate, w_up, w_down)


def solution(mesh):
    placed = (P(("pts", "head"), None), P(), P(), P(), P(), P(), P(), P(), P(), P("pts", None))
    return jax.shard_map(
        body, mesh=mesh, in_specs=placed, out_specs=P(("pts", "head"), None), check_vma=False
    )
```

```python
import functools
import math

import jax
import jax.numpy as jnp
from jax import lax
from jax.experimental import pallas as pl
from jax.experimental.pallas import tpu as pltpu
from jax.sharding import PartitionSpec as P


HEADS = 16
KV_HEADS = 4
HEAD_DIM = 64
BALL = 256
BLOCK = 128
CMP = 64
PICKS = 4
CAP = 2
EPS = 1e-06
LOG2E = math.log2(math.e)

ROWS = 512
PTS = 32
ZS = 4
BLK_DEV = 16
GROUP_W = 256
PAIR_W = 128
RATIO = HEADS // KV_HEADS
SUM_LOCAL = ROWS // CMP
SUM_ROWS = KV_HEADS * SUM_LOCAL
PAY_ROWS = SUM_ROWS + 16
PER = ROWS // BLOCK
BALLS = ROWS // BALL
FFN = 2048
UNIT = 256
STEPS = 2
GROUPS = ((0,), (1,), (3, 2))


bf16 = jnp.bfloat16
f32 = jnp.float32
VMEM = pltpu.VMEM
SMEM = pltpu.SMEM
NT = (((1,), (1,)), ((), ()))


def whole(space):
    return pl.BlockSpec(memory_space=space)


def near_core(array):
    return pltpu.with_memory_space_constraint(array, VMEM)


def far_core(array):
    return pltpu.with_memory_space_constraint(array, pltpu.HBM)


def params(mib):
    return pltpu.CompilerParams(vmem_limit_bytes=mib * 1024 * 1024)


def cost(flops, moved):
    return pl.CostEstimate(flops=flops, bytes_accessed=moved, transcendentals=0)


def head_ones(width):
    r = lax.broadcasted_iota(jnp.int32, (width, width), 0) // HEAD_DIM
    c = lax.broadcasted_iota(jnp.int32, (width, width), 1) // HEAD_DIM
    return jnp.where(r == c, 1.0, 0.0).astype(bf16)


def head_norm(raw, ones):
    squares = raw * raw
    high = squares.astype(bf16)
    low = (squares - high.astype(f32)).astype(bf16)
    sums = jnp.dot(high, ones, preferred_element_type=f32) + jnp.dot(
        low, ones, preferred_element_type=f32
    )
    return raw * lax.rsqrt(sums * (1.0 / HEAD_DIM) + EPS)


def row_norm(x):
    return x * lax.rsqrt(jnp.mean(x * x, axis=-1, keepdims=True) + EPS)


def first_body(
    z, picks_in, tokens_in, key_in, value_in,
    c0, c1, c2, c3, payload_out, normed_out, slots,
    table, tokens, w_key, w_value, normed, keys_held, values_held, pairs, payload, picks, sems, out_sem,
):
    rows_n = ROWS // STEPS
    weight_copies = [
        pltpu.make_async_copy(key_in, w_key, sems.at[0]),
        pltpu.make_async_copy(value_in, w_value, sems.at[1]),
    ]
    token_copies = [
        pltpu.make_async_copy(
            tokens_in.at[pl.ds(i * rows_n, rows_n)],
            tokens.at[pl.ds(i * rows_n, rows_n)],
            sems.at[2 + i],
        )
        for i in range(STEPS)
    ]
    picks_copy = pltpu.make_async_copy(picks_in, picks, out_sem.at[1])
    picks_copy.start()
    token_copies[0].start()
    weight_copies[0].start()
    weight_copies[1].start()
    for c in token_copies[1:]:
        c.start()

    def clear(i, _):
        table[i] = -1
        return 0

    lax.fori_loop(0, PTS * CAP, clear, 0, unroll=8)

    def assign(i, _):
        row = i // PICKS
        col = i % PICKS
        pick = picks[col, row]
        owner = pick // BLK_DEV
        offset = pick % BLK_DEV
        first = table[owner * CAP]
        slot = jnp.where((first == offset) | (first == -1), 0, 1)
        table[owner * CAP + slot] = offset
        slots[row, col] = owner * CAP + slot
        return 0

    picks_copy.wait()
    lax.fori_loop(0, BLK_DEV * PICKS, assign, 0, unroll=4)

    ones = head_ones(GROUP_W)
    key_means, value_means = [], []
    for i in range(STEPS):
        rows = pl.ds(i * rows_n, rows_n)
        token_copies[i].wait()
        here = row_norm(tokens[rows].astype(f32)).astype(bf16)
        normed[rows] = here
        if i == STEPS - 1:
            normed_copy = pltpu.make_async_copy(normed, normed_out, out_sem.at[2])
            normed_copy.start()
        if i == 0:
            weight_copies[0].wait()
        keys = jnp.dot(here, w_key[...], preferred_element_type=f32)
        keys = head_norm(keys, ones).astype(bf16)
        if i == 0:
            weight_copies[1].wait()
        values = jnp.dot(here, w_value[...], preferred_element_type=f32).astype(bf16)
        runs = (rows_n // CMP, CMP, GROUP_W)
        key_means.append(jnp.mean(keys.astype(f32).reshape(runs), axis=1))
        value_means.append(jnp.mean(values.astype(f32).reshape(runs), axis=1))
        keys_held[rows] = keys
        values_held[rows] = values
    summary_key = head_norm(jnp.concatenate(key_means, axis=0), ones)
    summary_value = jnp.concatenate(value_means, axis=0)
    summary = jnp.concatenate(
        [
            jnp.concatenate(
                [
                    summary_key[:, g * HEAD_DIM : (g + 1) * HEAD_DIM],
                    summary_value[:, g * HEAD_DIM : (g + 1) * HEAD_DIM],
                ],
                axis=1,
            )
            for g in range(KV_HEADS)
        ],
        axis=0,
    ).astype(bf16)
    lane = lax.broadcasted_iota(jnp.int32, (16, PAIR_W), 1)
    for o in range(PTS):
        payload[o, :SUM_ROWS, :] = summary
        first = jnp.maximum(table[o * CAP], 0)
        second = jnp.maximum(table[o * CAP + 1], 0)
        payload[o, SUM_ROWS:, :] = jnp.where(lane == 0, first, second).astype(f32).astype(bf16)
    told = pltpu.make_async_copy(payload, payload_out, out_sem.at[0])
    told.start()
    for g in range(KV_HEADS):
        lanes = slice(g * HEAD_DIM, (g + 1) * HEAD_DIM)
        pairs[g] = jnp.concatenate([keys_held[:, lanes], values_held[:, lanes]], axis=1)
    for k, c in enumerate((c0, c1, c2, c3)):
        c[...] = pairs[(z[0] + k) % ZS]
    told.wait()
    normed_copy.wait()


def first_stage(z, picks, tokens, w_key, w_value):
    hbm = whole(pltpu.HBM)
    return pl.pallas_call(
        first_body,
        name="first_stage",
        in_specs=[whole(SMEM)] + [hbm] * 4,
        out_specs=[whole(VMEM)] * ZS + [hbm, hbm, whole(SMEM)],
        out_shape=[VMEM((ROWS, PAIR_W), bf16)] * ZS
        + [
            pltpu.HBM((PTS, PAY_ROWS, PAIR_W), bf16),
            pltpu.HBM((ROWS, 1024), bf16),
            jax.ShapeDtypeStruct((BLK_DEV, PICKS), jnp.int32),
        ],
        scratch_shapes=[
            SMEM((PTS * CAP,), jnp.int32),
            VMEM((ROWS, 1024), bf16),
            VMEM((1024, GROUP_W), bf16),
            VMEM((1024, GROUP_W), bf16),
            VMEM((ROWS, 1024), bf16),
            VMEM((ROWS, GROUP_W), bf16),
            VMEM((ROWS, GROUP_W), bf16),
            VMEM((KV_HEADS, ROWS, PAIR_W), bf16),
            VMEM((PTS, PAY_ROWS, PAIR_W), bf16),
            SMEM((PICKS, BLK_DEV), jnp.int32),
            pltpu.SemaphoreType.DMA((2 + STEPS,)),
            pltpu.SemaphoreType.DMA((3,)),
        ],
        compiler_params=params(16),
        cost_estimate=cost(2 * ROWS * 1024 * 512, 4 << 20),
    )(z, *[far_core(a) for a in (picks, tokens, w_key, w_value)])


def q_body(z, normed_in, w_query, q0, q1, q2, q3, normed, raw, queries, sems):
    half = ROWS // 2
    ins = [
        pltpu.make_async_copy(
            normed_in.at[pl.ds(i * half, half)], normed.at[pl.ds(i * half, half)], sems.at[ZS + i]
        )
        for i in range(2)
    ]
    for c in ins:
        c.start()
    ones = head_ones(GROUP_W)

    def project(k, rows):
        start = pl.multiple_of(((z[0] + k) % ZS) * GROUP_W, GROUP_W)
        raw[k % 2, rows] = jnp.dot(
            normed[rows], w_query[:, pl.ds(start, GROUP_W)], preferred_element_type=f32
        )

    for i in range(2):
        ins[i].wait()
        project(0, slice(i * half, (i + 1) * half))
    outs = []
    for k, out in enumerate((q0, q1, q2, q3)):
        if k + 1 < ZS:
            project(k + 1, slice(0, ROWS))
        queries[k] = head_norm(raw[k % 2], ones).astype(bf16)
        outs.append(pltpu.make_async_copy(queries.at[k], out, sems.at[k]))
        outs[-1].start()
    for c in outs:
        c.wait()


def q_stage(z, normed, w_query):
    hbm = whole(pltpu.HBM)
    return pl.pallas_call(
        q_body,
        name="q_stage",
        in_specs=[whole(SMEM), hbm, whole(VMEM)],
        out_specs=[hbm] * ZS,
        out_shape=[pltpu.HBM((ROWS, GROUP_W), bf16)] * ZS,
        scratch_shapes=[
            VMEM((ROWS, 1024), bf16),
            VMEM((2, ROWS, GROUP_W), f32),
            VMEM((ZS, ROWS, GROUP_W), bf16),
            pltpu.SemaphoreType.DMA((ZS + 2,)),
        ],
        compiler_params=params(12),
        cost_estimate=cost(2 * ROWS * 1024 * 1024, 4 << 20),
    )(z, far_core(normed), near_core(w_query))


def reply_body(
    z, told, c0, c1, c2, c3, replies, s0, s1, s2, s3, kv_out, held, sums, asked_v, asked, sems, sum_sems
):
    asked_v[...] = told[:, SUM_ROWS, :].astype(f32).astype(jnp.int32)
    fetch = pltpu.make_async_copy(asked_v, asked, sum_sems.at[ZS])
    fetch.start()
    for k, c in enumerate((c0, c1, c2, c3)):
        held[k] = c[...].reshape(PER, BLOCK, PAIR_W)
    outs = [pltpu.make_async_copy(held, kv_out, sum_sems.at[ZS + 1])]
    outs[0].start()
    for k, s in enumerate((s0, s1, s2, s3)):
        start = pl.multiple_of(((z[0] + k) % ZS) * SUM_LOCAL, SUM_LOCAL)
        sums[k] = told[:, pl.ds(start, SUM_LOCAL), :].reshape(PTS * SUM_LOCAL, PAIR_W)
        outs.append(pltpu.make_async_copy(sums.at[k], s, sum_sems.at[k]))
        outs[-1].start()
    fetch.wait()

    def copy(i):
        b = asked[i // CAP, i % CAP]
        k = (z[0] - b // PER + ZS) % ZS
        return pltpu.make_async_copy(held.at[k, b % PER], replies.at[i], sems.at[i])

    def start_one(i, _):
        copy(i).start()
        return 0

    def wait_one(i, _):
        copy(i).wait()
        return 0

    lax.fori_loop(0, PTS * CAP, start_one, 0, unroll=4)
    lax.fori_loop(0, PTS * CAP, wait_one, 0, unroll=4)
    for c in outs:
        c.wait()


def reply_stage(z, told, chunks):
    hbm = whole(pltpu.HBM)
    return pl.pallas_call(
        reply_body,
        name="reply_stage",
        in_specs=[whole(SMEM)] + [whole(VMEM)] * 5,
        out_specs=[hbm] * (ZS + 2),
        out_shape=[pltpu.HBM((PTS * CAP, BLOCK, PAIR_W), bf16)]
        + [pltpu.HBM((PTS * SUM_LOCAL, PAIR_W), bf16)] * ZS
        + [pltpu.HBM((ZS, PER, BLOCK, PAIR_W), bf16)],
        scratch_shapes=[
            VMEM((ZS, PER, BLOCK, PAIR_W), bf16),
            VMEM((ZS, PTS * SUM_LOCAL, PAIR_W), bf16),
            VMEM((PTS, PAIR_W), jnp.int32),
            SMEM((PTS, PAIR_W), jnp.int32),
            pltpu.SemaphoreType.DMA((PTS * CAP,)),
            pltpu.SemaphoreType.DMA((ZS + 2,)),
        ],
        compiler_params=params(8),
    )(z, near_core(told), *[near_core(c) for c in chunks])


def ones_beside(kv):
    return jnp.concatenate([jnp.ones((kv.shape[0], HEAD_DIM), kv.dtype), kv[:, HEAD_DIM:]], axis=1)


def near_body(chunks, z, scale, kv, s0, s1, s2, s3, *rest):
    n = len(chunks)
    qs, outs = rest[:n], rest[-6 - 2 * n : -6]
    held, q, state, peaks, sems, peak_sems = rest[-6:]
    sums = jnp.concatenate([s0[...], s1[...], s2[...], s3[...]], axis=0)
    sum_keys = sums[:, :HEAD_DIM]
    sum_values = ones_beside(sums)
    half = BALL // BLOCK

    def copies(c, b, r):
        return (
            pltpu.make_async_copy(state.at[c, b, r], outs[2 * c].at[b, r], sems.at[c, b, r]),
            pltpu.make_async_copy(peaks.at[c, b, r], outs[2 * c + 1].at[b, r], peak_sems.at[c, b, r]),
        )

    def one_chunk(c, here_of, chunk, start_copies):
        balls = [kv[chunk, pl.ds(b * half, half)].reshape(BALL, PAIR_W) for b in range(BALLS)]
        values = [ones_beside(ball) for ball in balls]
        units = [(b, r) for b in range(BALLS) for r in range(RATIO)]

        def scores(u):
            b, r = units[u]
            here = here_of(b, r)
            ball = lax.dot_general(
                here, balls[b][:, :HEAD_DIM], NT, preferred_element_type=f32
            )
            far = lax.dot_general(here, sum_keys, NT, preferred_element_type=f32)
            held[u % 2, :, :BALL] = ball
            held[u % 2, :, BALL:] = far
            peak = jnp.maximum(
                jnp.max(ball, axis=1, keepdims=True), jnp.max(far, axis=1, keepdims=True)
            )
            return peak.astype(bf16).astype(f32)

        peak = scores(0)
        for u, (b, r) in enumerate(units):
            coming = scores(u + 1) if u + 1 < len(units) else None
            factor = scale[z[0] * RATIO + r] * (LOG2E / math.sqrt(HEAD_DIM))
            w = jnp.exp2((held[u % 2] - peak) * factor).astype(bf16)
            peaks[c, b, r] = jnp.broadcast_to(peak, (BALL, PAIR_W)).astype(bf16)
            state[c, b, r] = jnp.dot(w[:, :BALL], values[b], preferred_element_type=f32) + jnp.dot(
                w[:, BALL:], sum_values, preferred_element_type=f32
            )
            start_copies(b, r)
            peak = coming

    def part(ref):
        def take(b, r):
            return ref[b * BALL : (b + 1) * BALL, r * HEAD_DIM : (r + 1) * HEAD_DIM]

        return take

    if n == 1:

        def begin(b, r):
            for c in copies(0, b, r):
                c.start()

        one_chunk(0, part(qs[0]), chunks[0], begin)
    else:

        def loop(c, _):
            for i in range(n):

                @pl.when(c == i)
                def _():
                    q[...] = qs[i][...]

            chunk = jnp.where(c == 0, chunks[0], chunks[1])
            one_chunk(c, part(q), chunk, lambda b, r: None)
            for i in range(n):

                @pl.when(c == i)
                def _():
                    for b in range(BALLS):
                        for r in range(RATIO):
                            for m in copies(i, b, r):
                                m.start()

            return 0

        lax.fori_loop(0, n, loop, 0)
    for c in range(n):
        for b in range(BALLS):
            for r in range(RATIO):
                for m in copies(c, b, r):
                    m.wait()


def near_stage(chunks, z, scale, qs, kv, sums, others):
    n = len(chunks)
    shape = (BALLS, RATIO, BALL, PAIR_W)
    outs = pl.pallas_call(
        functools.partial(near_body, chunks),
        name="near_stage",
        in_specs=[whole(SMEM)] * 2 + [whole(VMEM)] * (5 + n) + [whole(pl.ANY)] * len(others),
        out_specs=[whole(pltpu.HBM)] * (2 * n),
        out_shape=[pltpu.HBM(shape, f32), pltpu.HBM(shape, bf16)] * n,
        scratch_shapes=[
            VMEM((2, BALL, BALL + PTS * SUM_LOCAL * ZS), f32),
            VMEM((ROWS if n > 1 else 16, GROUP_W), bf16),
            VMEM((n, *shape), f32),
            VMEM((n, *shape), bf16),
            pltpu.SemaphoreType.DMA((n, BALLS, RATIO)),
            pltpu.SemaphoreType.DMA((n, BALLS, RATIO)),
        ],
        compiler_params=params(14),
        cost_estimate=cost(8 * 4 * n * ROWS * 1280 * 64, 2 << 20),
    )(
        z,
        scale,
        near_core(kv),
        *[near_core(s) for s in sums],
        *[near_core(q) for q in qs],
        *[far_core(a) for a in others],
    )
    return [outs[2 * c : 2 * c + 2] for c in range(n)]


def far_body(shift_by, direct, z, slots, scale, q, state, peaks, fetched, *rest):
    if direct:
        out, held, state_held, peaks_held, sems = rest[-5:]
        brought = []
        for b in range(BALLS):
            brought.append(
                (
                    pltpu.make_async_copy(state.at[b], state_held.at[b], sems.at[b, 0]),
                    pltpu.make_async_copy(peaks.at[b], peaks_held.at[b], sems.at[b, 1]),
                )
            )
            for c in brought[-1]:
                c.start()
        state, peaks = state_held, peaks_held
    else:
        out, held = rest[-2:]
    lane = lax.broadcasted_iota(jnp.int32, (BLOCK, PAIR_W), 1)
    first_row = ((z[0] - shift_by + ZS) % ZS) * PER

    def part(r):
        return slice(r * BLOCK, (r + 1) * BLOCK)

    def keys_of(i):
        return jnp.concatenate([fetched[slots[first_row + i, j]] for j in range(PICKS)], axis=0)

    def scores(i, slot):
        here = jnp.concatenate(
            [q[pl.ds(i * BLOCK, BLOCK), r * HEAD_DIM : (r + 1) * HEAD_DIM] for r in range(RATIO)],
            axis=0,
        )
        s = lax.dot_general(here, keys_of(i)[:, :HEAD_DIM], NT, preferred_element_type=f32)
        held[slot] = s
        return jnp.max(s, axis=1, keepdims=True)

    def finish(b, i, slot, peak):
        rows = slice(slot * BLOCK, (slot + 1) * BLOCK)
        weights, keeps = [], []
        for r in range(RATIO):
            factor = scale[z[0] * RATIO + r] * (LOG2E / math.sqrt(HEAD_DIM))
            before = peaks[b, r, rows, :].astype(f32)
            new = jnp.maximum(before, peak[part(r)])
            s = held[slot, part(r), :]
            weights.append(
                jnp.concatenate(
                    [
                        jnp.exp2((s[:, part(j)] - new) * factor).astype(bf16)
                        for j in range(PICKS)
                    ],
                    axis=1,
                )
            )
            keeps.append(jnp.exp2((before - new) * factor))
        o = jnp.dot(
            jnp.concatenate(weights, axis=0), ones_beside(keys_of(i)), preferred_element_type=f32
        )
        for r in range(0, RATIO, 2):
            even = state[b, r, rows, :] * keeps[r] + o[part(r)]
            odd = state[b, r + 1, rows, :] * keeps[r + 1] + o[part(r + 1)]
            total = jnp.where(lane < HEAD_DIM, even, pltpu.roll(odd, HEAD_DIM, 1))
            summed = jnp.where(lane < HEAD_DIM, pltpu.roll(even, HEAD_DIM, 1), odd)
            out[pl.ds(i * BLOCK, BLOCK), r * HEAD_DIM : (r + 2) * HEAD_DIM] = (
                summed / total
            ).astype(bf16)

    def one_ball(b, peak):
        coming = scores(2 * b + 1, 1)
        finish(b, 2 * b, 0, peak)
        after = scores(2 * b + 2, 0) if b + 1 < BALLS else None
        if direct and b + 1 < BALLS:
            for c in brought[b + 1]:
                c.wait()
        finish(b, 2 * b + 1, 1, coming)
        return after

    peak = scores(0, 0)
    if direct:
        for c in brought[0]:
            c.wait()
    for b in range(BALLS):
        peak = one_ball(b, peak)


def far_stage(shift_by, z, slots, scale, q, state, fetched, others, direct=False):
    shape = (BALLS, RATIO, BALL, PAIR_W)
    place, keep = (pltpu.HBM, far_core) if direct else (VMEM, near_core)
    extra = [VMEM(shape, f32), VMEM(shape, bf16), pltpu.SemaphoreType.DMA((BALLS, 2))]
    return pl.pallas_call(
        functools.partial(far_body, shift_by, direct),
        name="far_stage",
        in_specs=[whole(SMEM)] * 3
        + [whole(VMEM)]
        + [whole(place)] * 2
        + [whole(VMEM)]
        + [whole(pl.ANY)] * len(others),
        out_specs=whole(VMEM),
        out_shape=VMEM((ROWS, GROUP_W), bf16),
        scratch_shapes=[VMEM((2, RATIO * BLOCK, PICKS * BLOCK), f32)] + (extra if direct else []),
        compiler_params=params(12),
        cost_estimate=cost(8 * 4 * ROWS * 512 * 64, 4 << 20),
    )(
        z,
        slots,
        scale,
        near_core(q),
        *[keep(a) for a in state],
        near_core(fetched),
        *[far_core(a) for a in others],
    )


def projected(z, k, part, w_out):
    start = pl.multiple_of(((z[0] + k) % ZS) * GROUP_W, GROUP_W)
    return jnp.dot(part[...], w_out[pl.ds(start, GROUP_W), :], preferred_element_type=f32)


def mid_body(z, tokens, a0, a1, a2, w_out, out):
    mid = tokens[...].astype(f32)
    for k, a in enumerate((a0, a1, a2)):
        mid = mid + projected(z, k, a, w_out)
    out[...] = mid


def mid_stage(z, tokens, parts, w_out):
    return pl.pallas_call(
        mid_body,
        name="mid_stage",
        in_specs=[whole(SMEM)] + [whole(VMEM)] * 5,
        out_specs=whole(VMEM),
        out_shape=VMEM((ROWS, 1024), f32),
        compiler_params=params(8),
        cost_estimate=cost(2 * ROWS * 1024 * 768, 4 << 20),
    )(z, *[near_core(a) for a in (tokens, *parts, w_out)])


def ffn_body(z, mid_in, a3, w_out, w_gate, w_up, w_down, out, mid_held, held, hidden):
    mid = mid_in[...] + projected(z, 3, a3, w_out)
    mid_held[...] = mid
    held[...] = row_norm(mid).astype(bf16)
    for j in range(FFN // UNIT):
        cols = slice(j * UNIT, (j + 1) * UNIT)
        gate = jnp.dot(held[...], w_gate[:, cols], preferred_element_type=f32)
        upward = jnp.dot(held[...], w_up[:, cols], preferred_element_type=f32)
        hidden[:, cols] = (gate / (1.0 + jnp.exp(-gate)) * upward).astype(bf16)
    out[...] = (
        mid_held[...] + jnp.dot(hidden[...], w_down[...], preferred_element_type=f32)
    ).astype(bf16)


def ffn_stage(z, mid, part, w_out, w_gate, w_up, w_down):
    return pl.pallas_call(
        ffn_body,
        name="ffn_stage",
        in_specs=[whole(SMEM)] + [whole(VMEM)] * 6,
        out_specs=whole(VMEM),
        out_shape=jax.ShapeDtypeStruct((ROWS, 1024), bf16),
        scratch_shapes=[VMEM((ROWS, 1024), f32), VMEM((ROWS, 1024), bf16), VMEM((ROWS, FFN), bf16)],
        compiler_params=params(14),
        cost_estimate=cost(2 * ROWS * 1024 * 6400, 18 << 20),
    )(z, *[near_core(a) for a in (mid, part, w_out, w_gate, w_up, w_down)])


def shift(array, k):
    return lax.ppermute(array, "head", [(i, (i + k) % ZS) for i in range(ZS)])


def body(tokens, w_query, w_key, w_value, w_out, logit_scale, w_gate, w_up, w_down, picks):
    z = lax.axis_index("head").astype(jnp.int32).reshape(1)
    *pairs, payload, normed, slots = first_stage(z, picks.T, tokens, w_key, w_value)
    chunks = [pairs[0], None, None, None]
    for k in (2, 1, 3):
        chunks[k] = shift(pairs[k], k)
    told = lax.all_to_all(payload, "pts", split_axis=0, concat_axis=0, tiled=True)
    query = q_stage(z, normed, w_query)
    replies, *sums, kv = reply_stage(z, told, chunks)
    replies = replies.reshape(PTS, CAP * BLOCK, PAIR_W)
    fetched = lax.all_to_all(replies, "pts", split_axis=0, concat_axis=0, tiled=True)
    fetched = fetched.reshape(PTS * CAP, BLOCK, PAIR_W)
    sums = [sums[0]] + [shift(sums[k], k) for k in (1, 2, 3)]
    q = [query[0], None, None, None]
    for k in (1, 3, 2):
        q[k] = shift(query[k], k)
    states = [None] * ZS
    done = []
    for group in GROUPS:
        rows = pairs[0].reshape(1, PER, BLOCK, PAIR_W) if group == (0,) else kv
        made = near_stage(group, z, logit_scale, [q[k] for k in group], rows, sums, done)
        for k, one in zip(group, made):
            states[k] = one
        done = made[-1]
    parts = [None] * ZS
    for k in (2, 1, 3, 0):
        others = states[2] if k != 2 else []
        attended = far_stage(k, z, slots, logit_scale, q[k], states[k], fetched, others, k == 2)
        parts[k] = shift(attended, ZS - k) if k else attended
    mid = mid_stage(z, tokens, parts[:3], w_out)
    return ffn_stage(z, mid, parts[3], w_out, w_gate, w_up, w_down)


def solution(mesh):
    placed = (P(("pts", "head"), None), P(), P(), P(), P(), P(), P(), P(), P(), P("pts", None))
    return jax.shard_map(
        body, mesh=mesh, in_specs=placed, out_specs=P(("pts", "head"), None), check_vma=False
    )
```
